256 devices in a mesh: win: 16 (over x, y), dof: 16 (over z, core).
Axes of the slice: x: 4, y: 4, z: 8, core: 2. Of those that a mesh axis runs over, the one named last changes fastest.
Arguments:
- snapshots: bfloat16 [524288, 1024], P('dof', 'win'), may hold values from -6 to 6
- sketch_matrix: bfloat16 [524288, 128], P('dof'), may hold values from -0.0078125 to 0.0078125
- pivots: int32 [32, 64], P('win'), may hold values from 0 to 127
Outputs:
- singular: float32 [32, 64], P('win')
- projections: float32 [32, 64, 32], P('win')
The draws below stay inside these ranges and needn't reach their ends.
All inputs are finite; a program needn't handle non-finite values.
Results may differ from the reference program's by a relative error of at most 0.0003.
Values sent between devices are 32-bit elements; how exact they have to be, the bound alone decides.
A program may use at most 64 MiB of HBM per device.

```python
import math
import jax
import jax.numpy as jnp
from jax import lax

SNAPS = 32
SKETCH = 128
RANK = 64
ORTH_ITERS = 2
WINDOWS = 32
DOFS = 524288


def set_ends(drawn, key, smallest, top_value):
    longest = drawn.shape.index(max(drawn.shape))
    spots = []
    for shift in (0, 1):
        where = [jax.random.randint(jax.random.fold_in(key, axis), (), 0, length) for axis, length in enumerate(drawn.shape)]
        where[longest] = (where[longest] + shift) % drawn.shape[longest]
        spots.append(tuple(where))
    return drawn.at[spots[0]].set(smallest).at[spots[1]].set(top_value)


def block_levels(stream_key, dims, cuts, least, largest):
    def one(axis_at, shards_of):
        steps = jax.random.uniform(jax.random.fold_in(jax.random.fold_in(stream_key, 6), axis_at), (shards_of,), jnp.float32, least / len(cuts), largest / len(cuts))
        return jnp.repeat(jnp.exp(steps), dims[axis_at] // shards_of).reshape((-1,) + (1,) * (len(dims) - axis_at - 1))

    gain = one(*cuts[0])
    for cut in cuts[1:]:
        gain = gain * one(*cut)
    return gain


def centred(stream_key, dims, width, reach, cuts=(), kind=jnp.bfloat16):
    array = width * jax.random.normal(stream_key, dims, jnp.float32)
    if cuts:
        array = array * block_levels(stream_key, dims, cuts, -0.22, 0.18)
    return jnp.clip(array, -reach, reach).astype(kind)


def setup_inputs(seed: int = 0) -> dict:
    key_of = jax.random.split(jax.random.key(seed), 4)
    snapshots = centred(key_of[0], (DOFS, WINDOWS * SNAPS), 1.0, 6.0, ((0, 16), (1, 16)))
    sketch_matrix = centred(key_of[1], (DOFS, SKETCH), DOFS ** -0.5, 0.0078125, ((0, 16),))
    pivots = set_ends(jax.random.randint(key_of[2], (WINDOWS, RANK), 0, SKETCH), jax.random.fold_in(key_of[2], 1), 0, SKETCH - 1).astype(jnp.int32)
    return {"snapshots": snapshots, "sketch_matrix": sketch_matrix, "pivots": pivots}


HIGHEST_PREC = lax.Precision.HIGHEST

def orthogonal(prefix_grams):
    batch_count = prefix_grams.shape[0]
    sketch_width = prefix_grams.shape[1]
    basis_cols = jnp.broadcast_to(jnp.eye(sketch_width, RANK, dtype=jnp.float32), (batch_count, sketch_width, RANK))
    for sweep_index in range(ORTH_ITERS):
        images = jnp.einsum('wij,wjk->wik', prefix_grams, basis_cols, precision=HIGHEST_PREC)
        inner_gram = jnp.einsum('wik,wil->wkl', images, images, precision=HIGHEST_PREC)
        chol_factor = jnp.linalg.cholesky(inner_gram)
        solved = jax.scipy.linalg.solve_triangular(chol_factor, jnp.swapaxes(images, 1, 2), lower=True)
        basis_cols = jnp.swapaxes(solved, 1, 2)
    return basis_cols

def finish(prefix_grams, basis_cols, window_blocks, pivots):
    images = jnp.einsum('wij,wjk->wik', prefix_grams, basis_cols, precision=HIGHEST_PREC)
    singular = jnp.sqrt(lax.optimization_barrier(jnp.sum(basis_cols * images, axis=1)))
    sketch_width = basis_cols.shape[1]
    pivot_table = (pivots[:, :, None] == jnp.arange(sketch_width, dtype=jnp.int32)[None, None, :]).astype(jnp.float32)
    pivot_weight = jnp.einsum('wrk,wkr->wr', pivot_table, basis_cols, precision=HIGHEST_PREC) * math.sqrt(sketch_width)
    projections = jnp.einsum('wkr,wks->wrs', basis_cols, window_blocks, precision=HIGHEST_PREC) * pivot_weight[:, :, None]
    return (singular, projections)

def reference(snapshots, sketch_matrix, pivots):
    coefficients = jnp.dot(sketch_matrix.T.astype(jnp.float32), snapshots.astype(jnp.float32), preferred_element_type=jnp.float32)
    window_blocks = jnp.transpose(coefficients.reshape(SKETCH, WINDOWS, SNAPS), (1, 0, 2))
    window_grams = jnp.einsum('wks,wjs->wkj', window_blocks, window_blocks, precision=HIGHEST_PREC)
    own_prefix = jnp.cumsum(window_grams, axis=0)
    snap_totals = (SNAPS * (jnp.arange(WINDOWS, dtype=jnp.int32) + 1)).astype(jnp.float32)
    identity = jnp.eye(SKETCH, dtype=jnp.float32)
    prefix_grams = identity[None] + own_prefix / snap_totals[:, None, None]
    basis_cols = orthogonal(prefix_grams)
    singular, projections = finish(prefix_grams, basis_cols, window_blocks, pivots)
    return (singular, projections)
```

```python
import functools
import math

import jax
import jax.numpy as jnp
from jax import lax
from jax.experimental import pallas as pl
from jax.experimental.pallas import tpu as pltpu
from jax.sharding import PartitionSpec as P

HIGHEST_PREC = lax.Precision.HIGHEST
RANK = 64
NT = (((1,), (1,)), ((), ()))


def dot_nt(a, b):
    return lax.dot_general(a, b, NT, precision=HIGHEST_PREC, preferred_element_type=jnp.float32)


def dot_nn(a, b):
    return lax.dot_general(a, b, (((1,), (0,)), ((), ())), precision=HIGHEST_PREC, preferred_element_type=jnp.float32)


def halves(a, b):
    return jnp.concatenate([a[:, :64], b[:, :64]], axis=1), jnp.concatenate([a[:, 64:], b[:, 64:]], axis=1)


def split_rows(x):
    return [x[8 * i : 8 * i + 8, :] for i in range(8)]


def whiten(gram, low, high):
    lane = lax.broadcasted_iota(jnp.int32, (8, 128), 1)
    sub = lax.broadcasted_iota(jnp.int32, (8, 128), 0)
    base = lane - lane % 64
    v0, v1, v2 = split_rows(gram), split_rows(low), split_rows(high)
    for kb in range(8):
        cols = []
        for j in range(8):
            idx = base + (8 * kb + j)
            cols.append({i: jnp.take_along_axis(v0[i], idx, axis=1) for i in range(kb, 8)})
        diag = cols[0][kb]
        for p in range(8):
            pivot = jnp.broadcast_to(cols[p][kb][p : p + 1, :], (8, 128))
            if p:
                diag = jnp.where(sub >= p, pivot, diag)
            else:
                diag = pivot
            inv = 1.0 / pivot
            mult = {i: cols[p][i] * inv for i in range(kb, 8)}
            mult[kb] = jnp.where(sub > p, mult[kb], 0.0)
            for j in range(p + 1, 8):
                row = jnp.broadcast_to(cols[j][kb][p : p + 1, :], (8, 128))
                for i in range(kb, 8):
                    cols[j][i] = cols[j][i] - mult[i] * row
            for v in (v0, v1, v2) if kb < 7 else (v1, v2):
                row = jnp.broadcast_to(v[kb][p : p + 1, :], (8, 128))
                for i in range(kb, 8):
                    v[i] = v[i] - mult[i] * row
        scale = lax.rsqrt(diag)
        v1[kb] = v1[kb] * scale
        v2[kb] = v2[kb] * scale
    return jnp.concatenate(v1, axis=0), jnp.concatenate(v2, axis=0)


def masked_pair(low, high):
    first = lax.broadcasted_iota(jnp.int32, (64, 128), 1) < 64
    zero = jnp.zeros((64, 128), jnp.float32)
    top = jnp.concatenate([jnp.where(first, low, zero), jnp.where(first, high, zero)], axis=1)
    bottom = jnp.concatenate([jnp.where(first, zero, low), jnp.where(first, zero, high)], axis=1)
    return jnp.concatenate([top, bottom], axis=0)


def solve_windows(pa, pb, za, zb, pivots_row):
    alo, ahi = halves(pa, pb)
    zero = jnp.zeros((64, 64), jnp.float32)

    def block_rows(x, first):
        left = jnp.concatenate([x[:, :64], zero] if first else [zero, x[:, 64:]], axis=1)
        return left

    lo_a, lo_b = alo[:64], alo[64:]
    hi_a, hi_b = ahi[:64], ahi[64:]
    joint = jnp.concatenate(
        [
            jnp.concatenate([block_rows(lo_a, True), block_rows(hi_a, True)], axis=1),
            jnp.concatenate([block_rows(lo_a, False), block_rows(hi_a, False)], axis=1),
            jnp.concatenate([block_rows(lo_b, True), block_rows(hi_b, True)], axis=1),
            jnp.concatenate([block_rows(lo_b, False), block_rows(hi_b, False)], axis=1),
        ],
        axis=0,
    )
    low, high = lo_a, hi_a
    for sweep in range(2):
        if sweep:
            image = dot_nn(jnp.concatenate([low, high], axis=1), joint)
            low, high = image[:, :128], image[:, 128:]
        gram = dot_nt(jnp.concatenate([low, high], axis=1), masked_pair(low, high))
        low, high = whiten(gram, low, high)
    basis = jnp.concatenate([low, high], axis=1)
    image = dot_nn(basis, joint)
    prod = basis * image
    first = lax.broadcasted_iota(jnp.int32, (8, 256), 1) % 128 < 64
    row = lax.broadcasted_iota(jnp.int32, (8, 256), 0)
    pick = jnp.where((row == 0) & first, 1.0, 0.0) + jnp.where((row == 1) & (~first), 1.0, 0.0)
    squares = dot_nt(pick, prod)
    j = lax.broadcasted_iota(jnp.int32, (256, 128), 0)
    lane = lax.broadcasted_iota(jnp.int32, (256, 128), 1)
    own = (j // 64) % 2 == lane // 64
    dim = j % 64 + 64 * (j // 128)
    onehot = jnp.where(own & (dim == pivots_row), 1.0, 0.0)
    picked = dot_nn(basis, onehot)
    r = lax.broadcasted_iota(jnp.int32, (64, 128), 0)
    c = lax.broadcasted_iota(jnp.int32, (64, 128), 1)
    weight = jnp.sum(jnp.where(c % 64 == r, picked, 0.0), axis=0, keepdims=True) * math.sqrt(128)
    zlo, zhi = halves(za, zb)
    proj = dot_nt(jnp.concatenate([zlo, zhi], axis=1), masked_pair(low, high)) * weight
    return jnp.sqrt(squares[:2]), proj


def ortho_kernel(grams_ref, y_ref, pivots_ref, sing_ref, proj_ref):
    piv = pivots_ref[...]
    piv_row = jnp.concatenate([piv[0:1, :], piv[1:2, :]], axis=1)
    sing, proj = solve_windows(grams_ref[0], grams_ref[1], y_ref[:32, :], y_ref[32:, :], piv_row)
    sing_ref[...] = sing
    proj_ref[0] = proj[:, :64]
    proj_ref[1] = proj[:, 64:]


def ortho_call(grams, yt, pivots):
    sing, proj = pl.pallas_call(
        ortho_kernel,
        out_shape=(jax.ShapeDtypeStruct((2, 64), jnp.float32), jax.ShapeDtypeStruct((2, 32, 64), jnp.float32)),
        in_specs=[pl.BlockSpec(memory_space=pltpu.VMEM)] * 3,
        out_specs=(pl.BlockSpec(memory_space=pltpu.VMEM),) * 2,
    )(grams, yt, pivots)
    return sing, jnp.swapaxes(proj, 1, 2)


def total_of_pieces(shard, axis):
    return lax.all_gather(shard, axis).sum(0)


def sent_to_all(shard, axis):
    peers = lax.axis_size(axis)
    return lax.all_to_all(
        jnp.broadcast_to(shard[None], (peers, *shard.shape)), axis, 0, 0, tiled=True
    )


def joined_along(parts, dim):
    parts = jnp.moveaxis(parts, 0, dim)
    lengths = parts.shape
    return parts.reshape(*lengths[:dim], lengths[dim] * lengths[dim + 1], *lengths[dim + 2 :])


def collect(shard, axis, dim):
    parts = sent_to_all(shard, axis)
    return joined_along(parts, dim)


def masked_gram(gathered, limit):
    column_ids = lax.iota(jnp.int32, gathered.shape[1])
    keep_mask = (column_ids < limit).astype(jnp.float32)
    return jnp.dot(gathered * keep_mask[None, :], gathered.T, precision=HIGHEST_PREC)


def local(snapshots, sketch_matrix, pivots):
    windows_here = pivots.shape[0]
    sketch_width = sketch_matrix.shape[1]
    local_cols = snapshots.shape[1]
    snap_count = local_cols // windows_here
    win_position = lax.axis_index("win")
    partial_value = lax.dot_general(
        sketch_matrix, snapshots, (((0,), (0,)), ((), ())), preferred_element_type=jnp.float32
    )
    coefficients = total_of_pieces(partial_value, "dof")
    window_blocks = jnp.transpose(
        coefficients.reshape(sketch_width, windows_here, snap_count), (1, 0, 2)
    )
    window_grams = jnp.einsum("wks,wjs->wkj", window_blocks, window_blocks, precision=HIGHEST_PREC)
    own_prefix = jnp.cumsum(window_grams, axis=0)
    gathered = collect(coefficients, "win", 1)
    earlier = masked_gram(gathered, win_position * local_cols)
    window_ids = win_position * windows_here + jnp.arange(windows_here, dtype=jnp.int32)
    snap_totals = (snap_count * (window_ids + 1)).astype(jnp.float32)
    identity = jnp.eye(sketch_width, dtype=jnp.float32)
    prefix_grams = identity[None] + (earlier[None] + own_prefix) / snap_totals[:, None, None]
    return ortho_call(prefix_grams, coefficients.T, pivots)


def solution(mesh):
    placed = (P("dof", "win"), P("dof", None), P("win", None))
    return jax.shard_map(
        local,
        mesh=mesh,
        in_specs=placed,
        out_specs=(P("win", None), P("win", None, None)),
        check_vma=False,
    )
```

```python
import functools
import math

import jax
import jax.numpy as jnp
from jax import lax
from jax.experimental import pallas as pl
from jax.experimental.pallas import tpu as pltpu
from jax.sharding import PartitionSpec as P

HIGHEST_PREC = lax.Precision.HIGHEST
RANK = 64
NT = (((1,), (1,)), ((), ()))


def dot_nt(a, b):
    return lax.dot_general(a, b, NT, precision=HIGHEST_PREC, preferred_element_type=jnp.float32)


def dot_nn(a, b):
    return lax.dot_general(a, b, (((1,), (0,)), ((), ())), precision=HIGHEST_PREC, preferred_element_type=jnp.float32)


def halves(a, b):
    return jnp.concatenate([a[:, :64], b[:, :64]], axis=1), jnp.concatenate([a[:, 64:], b[:, 64:]], axis=1)


def split_rows(x):
    return [x[8 * i : 8 * i + 8, :] for i in range(8)]


def whiten(gram, low, high):
    lane = lax.broadcasted_iota(jnp.int32, (8, 128), 1)
    sub = lax.broadcasted_iota(jnp.int32, (8, 128), 0)
    base = lane - lane % 64
    v0, v1, v2 = split_rows(gram), split_rows(low), split_rows(high)
    for kb in range(8):
        cols = []
        for j in range(8):
            idx = base + (8 * kb + j)
            cols.append({i: jnp.take_along_axis(v0[i], idx, axis=1) for i in range(kb, 8)})
        diag = cols[0][kb]
        for p in range(8):
            pivot = jnp.broadcast_to(cols[p][kb][p : p + 1, :], (8, 128))
            if p:
                diag = jnp.where(sub >= p, pivot, diag)
            else:
                diag = pivot
            inv = 1.0 / pivot
            mult = {i: cols[p][i] * inv for i in range(kb, 8)}
            mult[kb] = jnp.where(sub > p, mult[kb], 0.0)
            for j in range(p + 1, 8):
                row = jnp.broadcast_to(cols[j][kb][p : p + 1, :], (8, 128))
                for i in range(kb, 8):
                    cols[j][i] = cols[j][i] - mult[i] * row
            for v in (v0, v1, v2) if kb < 7 else (v1, v2):
                row = jnp.broadcast_to(v[kb][p : p + 1, :], (8, 128))
                for i in range(kb, 8):
                    v[i] = v[i] - mult[i] * row
        scale = lax.rsqrt(diag)
        v1[kb] = v1[kb] * scale
        v2[kb] = v2[kb] * scale
    return jnp.concatenate(v1, axis=0), jnp.concatenate(v2, axis=0)


def masked_pair(low, high):
    first = lax.broadcasted_iota(jnp.int32, (64, 128), 1) < 64
    zero = jnp.zeros((64, 128), jnp.float32)
    top = jnp.concatenate([jnp.where(first, low, zero), jnp.where(first, high, zero)], axis=1)
    bottom = jnp.concatenate([jnp.where(first, zero, low), jnp.where(first, zero, high)], axis=1)
    return jnp.concatenate([top, bottom], axis=0)


def solve_windows(pa, pb, za, zb, pivots_row):
    alo, ahi = halves(pa, pb)
    zero = jnp.zeros((64, 64), jnp.float32)

    def block_rows(x, first):
        left = jnp.concatenate([x[:, :64], zero] if first else [zero, x[:, 64:]], axis=1)
        return left

    lo_a, lo_b = alo[:64], alo[64:]
    hi_a, hi_b = ahi[:64], ahi[64:]
    joint = jnp.concatenate(
        [
            jnp.concatenate([block_rows(lo_a, True), block_rows(hi_a, True)], axis=1),
            jnp.concatenate([block_rows(lo_a, False), block_rows(hi_a, False)], axis=1),
            jnp.concatenate([block_rows(lo_b, True), block_rows(hi_b, True)], axis=1),
            jnp.concatenate([block_rows(lo_b, False), block_rows(hi_b, False)], axis=1),
        ],
        axis=0,
    )
    low, high = lo_a, hi_a
    for sweep in range(2):
        if sweep:
            image = dot_nn(jnp.concatenate([low, high], axis=1), joint)
            low, high = image[:, :128], image[:, 128:]
        gram = dot_nt(jnp.concatenate([low, high], axis=1), masked_pair(low, high))
        low, high = whiten(gram, low, high)
    basis = jnp.concatenate([low, high], axis=1)
    image = dot_nn(basis, joint)
    prod = basis * image
    first = lax.broadcasted_iota(jnp.int32, (8, 256), 1) % 128 < 64
    row = lax.broadcasted_iota(jnp.int32, (8, 256), 0)
    pick = jnp.where((row == 0) & first, 1.0, 0.0) + jnp.where((row == 1) & (~first), 1.0, 0.0)
    squares = dot_nt(pick, prod)
    j = lax.broadcasted_iota(jnp.int32, (256, 128), 0)
    lane = lax.broadcasted_iota(jnp.int32, (256, 128), 1)
    own = (j // 64) % 2 == lane // 64
    dim = j % 64 + 64 * (j // 128)
    onehot = jnp.where(own & (dim == pivots_row), 1.0, 0.0)
    picked = dot_nn(basis, onehot)
    r = lax.broadcasted_iota(jnp.int32, (64, 128), 0)
    c = lax.broadcasted_iota(jnp.int32, (64, 128), 1)
    weight = jnp.sum(jnp.where(c % 64 == r, picked, 0.0), axis=0, keepdims=True) * math.sqrt(128)
    zlo, zhi = halves(za, zb)
    proj = dot_nt(jnp.concatenate([zlo, zhi], axis=1), masked_pair(low, high)) * weight
    return jnp.sqrt(squares[:2]), proj


MESH = pl.DeviceIdType.MESH
CHUNKS = 16


def rdma(src, dst, send, recv, where):
    return pltpu.make_async_remote_copy(
        src_ref=src, dst_ref=dst, send_sem=send, recv_sem=recv, device_id=where, device_id_type=MESH
    )


def sum_kernel(stop, snap_hbm, sketch_hbm, own_ref, base_ref,
               snap, sketch, part, rs_buf, ag_buf, gath, gram_send, gram_recv,
               in_sem, rs_send, rs_recv, ag_send, ag_recv, xy_send, xy_recv, pair_sem):
    d = lax.axis_index("dof")
    w = lax.axis_index("win")
    nd, nw = 16, 16
    core = lax.rem(d, 2)
    depth = sketch.shape[1]
    loads = []
    for i in range(CHUNKS):
        a = pltpu.make_async_copy(sketch_hbm.at[pl.ds(i * depth, depth), :], sketch.at[i], in_sem.at[0, i])
        b = pltpu.make_async_copy(snap_hbm.at[:, pl.ds(i * depth, depth)], snap.at[i], in_sem.at[1, i])
        a.start()
        b.start()
        loads.append((a, b))
    gath[...] = jnp.zeros_like(gath)
    barrier = pltpu.get_barrier_semaphore()
    for k in range(1, 16):
        pl.semaphore_signal(barrier, inc=1, device_id={"dof": lax.rem(d + k, nd)}, device_id_type=MESH)
        pl.semaphore_signal(barrier, inc=1, device_id={"win": lax.rem(w + k, nw)}, device_id_type=MESH)
    total = jnp.zeros((64, 128), jnp.float32)
    for i in range(CHUNKS):
        for copy in loads[i]:
            copy.wait()
        total = total + jnp.dot(snap[i], sketch[i], preferred_element_type=jnp.float32)
    for p in range(16):
        part[p] = total[4 * p : 4 * p + 4, :]
    pl.semaphore_wait(barrier, 30)
    if stop < 1:
        own_ref[...] = total
        base_ref[...] = jnp.zeros_like(base_ref)
        return
    order = [8, 9, 7, 6, 10, 5, 11, 4, 12, 3, 13, 2, 14, 15, 1]
    sends = []
    for k in order:
        q = lax.rem(d + k, nd)
        copy = rdma(part.at[q], rs_buf.at[d], rs_send.at[k], rs_recv.at[d], {"dof": q})
        copy.start()
        sends.append(copy)
    rs_buf[d] = part[d]
    for k in reversed(order):
        q = lax.rem(d + k, nd)
        rdma(part.at[q], rs_buf.at[q], rs_send.at[k], rs_recv.at[q], {"dof": q}).wait_recv()
    ag_buf[d] = jnp.sum(rs_buf[...], axis=0)
    if stop >= 2:
        for k in order:
            q = lax.rem(d + k, nd)
            copy = rdma(ag_buf.at[d], ag_buf.at[d], ag_send.at[k], ag_recv.at[d], {"dof": q})
            copy.start()
            sends.append(copy)
    forwards = []

    def forward(k, q):
        z = q // 2
        for v in range(16):
            copy = rdma(ag_buf.at[q], gath.at[w, z], xy_send.at[k // 2, v], xy_recv.at[w, z], {"win": v})
            forwards.append((v, copy))

            @pl.when(v > w)
            def _():
                copy.start()

    if stop >= 3:
        forward(0, d)
    if stop >= 2:
        for k in reversed(order):
            q = lax.rem(d + k, nd)
            rdma(ag_buf.at[q], ag_buf.at[q], ag_send.at[k], ag_recv.at[q], {"dof": q}).wait_recv()
            if stop >= 3 and k % 2 == 0:
                forward(k, q)
    if stop >= 3:
        for v in range(16):
            @pl.when(v < w)
            def _():
                for z in range(8):
                    rdma(ag_buf.at[0], gath.at[v, z], xy_send.at[0, v], xy_recv.at[v, z], {"win": v}).wait_recv()
    own_ref[...] = ag_buf[...].reshape(64, 128)
    if stop >= 4:
        x = gath[...].reshape(512, 128)
        gram_send[...] = lax.dot_general(x, x, (((0,), (0,)), ((), ())), precision=lax.Precision.HIGHEST,
                                         preferred_element_type=jnp.float32)
        copy = rdma(gram_send, gram_recv, pair_sem.at[0], pair_sem.at[1], {"dof": d + 1 - 2 * core})
        copy.start()
        copy.wait()
        base_ref[...] = gram_send[...] + gram_recv[...]
    else:
        base_ref[...] = jnp.sum(gath[...].reshape(4, 128, 128), axis=0)
    for copy in sends:
        copy.wait_send()
    for v, copy in forwards:
        @pl.when(v > w)
        def _():
            copy.wait_send()


def sum_call(snapshots, sketch_matrix, stop=4):
    depth = sketch_matrix.shape[0] // CHUNKS
    f32 = jnp.float32
    return pl.pallas_call(
        functools.partial(sum_kernel, stop),
        out_shape=(jax.ShapeDtypeStruct((64, 128), f32), jax.ShapeDtypeStruct((128, 128), f32)),
        in_specs=[pl.BlockSpec(memory_space=pl.ANY)] * 2,
        out_specs=(pl.BlockSpec(memory_space=pltpu.VMEM),) * 2,
        scratch_shapes=[
            pltpu.VMEM((CHUNKS, 64, depth), jnp.bfloat16),
            pltpu.VMEM((CHUNKS, depth, 128), jnp.bfloat16),
            pltpu.VMEM((16, 4, 128), f32),
            pltpu.VMEM((16, 4, 128), f32),
            pltpu.VMEM((16, 4, 128), f32),
            pltpu.VMEM((16, 8, 4, 128), f32),
            pltpu.VMEM((128, 128), f32),
            pltpu.VMEM((128, 128), f32),
            pltpu.SemaphoreType.DMA((2, CHUNKS)),
            pltpu.SemaphoreType.DMA((16,)),
            pltpu.SemaphoreType.DMA((16,)),
            pltpu.SemaphoreType.DMA((16,)),
            pltpu.SemaphoreType.DMA((16,)),
            pltpu.SemaphoreType.DMA((8, 16)),
            pltpu.SemaphoreType.DMA((16, 8)),
            pltpu.SemaphoreType.DMA((2,)),
        ],
        compiler_params=pltpu.CompilerParams(collective_id=0, has_side_effects=True),
    )(snapshots.T, sketch_matrix)

def solve_kernel(own_ref, base_ref, pivots_ref, sing_ref, proj_ref):
    w = lax.axis_index("win")
    piv = pivots_ref[...]
    piv_row = jnp.concatenate([piv[0:1, :], piv[1:2, :]], axis=1)
    za, zb = own_ref[:32, :], own_ref[32:, :]
    ma = lax.dot_general(za, za, (((0,), (0,)), ((), ())), precision=HIGHEST_PREC, preferred_element_type=jnp.float32)
    mb = lax.dot_general(zb, zb, (((0,), (0,)), ((), ())), precision=HIGHEST_PREC, preferred_element_type=jnp.float32)
    eye = jnp.where(
        lax.broadcasted_iota(jnp.int32, (128, 128), 0) == lax.broadcasted_iota(jnp.int32, (128, 128), 1), 1.0, 0.0
    )
    count = jnp.full((128, 128), 64 * w, jnp.int32).astype(jnp.float32)
    sa = base_ref[...] + ma
    sb = sa + mb
    sing, proj = solve_windows(eye + sa / (count + 32.0), eye + sb / (count + 64.0), za, zb, piv_row)
    sing_ref[...] = sing
    proj_ref[0] = proj[:, :64]
    proj_ref[1] = proj[:, 64:]


def local(snapshots, sketch_matrix, pivots):
    own, base = sum_call(snapshots, sketch_matrix)
    sing, proj = pl.pallas_call(
        solve_kernel,
        out_shape=(jax.ShapeDtypeStruct((2, 64), jnp.float32), jax.ShapeDtypeStruct((2, 32, 64), jnp.float32)),
        in_specs=[pl.BlockSpec(memory_space=pltpu.VMEM)] * 3,
        out_specs=(pl.BlockSpec(memory_space=pltpu.VMEM),) * 2,
    )(own, base, pivots)
    return sing, jnp.swapaxes(proj, 1, 2)


def solution(mesh):
    placed = (P("dof", "win"), P("dof", None), P("win", None))
    return jax.shard_map(
        local,
        mesh=mesh,
        in_specs=placed,
        out_specs=(P("win", None), P("win", None, None)),
        check_vma=False,
    )
```

```python
import functools
import math

import jax
import jax.numpy as jnp
from jax import lax
from jax.experimental import pallas as pl
from jax.experimental.pallas import tpu as pltpu
from jax.sharding import PartitionSpec as P

HIGHEST_PREC = lax.Precision.HIGHEST
RANK = 64
NT = (((1,), (1,)), ((), ()))


def dot_nt(a, b):
    return lax.dot_general(a, b, NT, precision=HIGHEST_PREC, preferred_element_type=jnp.float32)


def dot_nn(a, b):
    return lax.dot_general(a, b, (((1,), (0,)), ((), ())), precision=HIGHEST_PREC, preferred_element_type=jnp.float32)


def halves(a, b):
    return jnp.concatenate([a[:, :64], b[:, :64]], axis=1), jnp.concatenate([a[:, 64:], b[:, 64:]], axis=1)


def split_rows(x):
    return [x[8 * i : 8 * i + 8, :] for i in range(8)]


def whiten(gram, low, high):
    lane = lax.broadcasted_iota(jnp.int32, (8, 128), 1)
    sub = lax.broadcasted_iota(jnp.int32, (8, 128), 0)
    base = lane - lane % 64
    v0, v1, v2 = split_rows(gram), split_rows(low), split_rows(high)
    for kb in range(8):
        cols = []
        for j in range(8):
            idx = base + (8 * kb + j)
            cols.append({i: jnp.take_along_axis(v0[i], idx, axis=1) for i in range(kb, 8)})
        diag = cols[0][kb]
        for p in range(8):
            pivot = jnp.broadcast_to(cols[p][kb][p : p + 1, :], (8, 128))
            if p:
                diag = jnp.where(sub >= p, pivot, diag)
            else:
                diag = pivot
            inv = 1.0 / pivot
            mult = {i: cols[p][i] * inv for i in range(kb, 8)}
            mult[kb] = jnp.where(sub > p, mult[kb], 0.0)
            for j in range(p + 1, 8):
                row = jnp.broadcast_to(cols[j][kb][p : p + 1, :], (8, 128))
                for i in range(kb, 8):
                    cols[j][i] = cols[j][i] - mult[i] * row
            for v in (v0, v1, v2) if kb < 7 else (v1, v2):
                row = jnp.broadcast_to(v[kb][p : p + 1, :], (8, 128))
                for i in range(kb, 8):
                    v[i] = v[i] - mult[i] * row
        scale = lax.rsqrt(diag)
        v1[kb] = v1[kb] * scale
        v2[kb] = v2[kb] * scale
    return jnp.concatenate(v1, axis=0), jnp.concatenate(v2, axis=0)


def masked_pair(low, high):
    first = lax.broadcasted_iota(jnp.int32, (64, 128), 1) < 64
    zero = jnp.zeros((64, 128), jnp.float32)
    top = jnp.concatenate([jnp.where(first, low, zero), jnp.where(first, high, zero)], axis=1)
    bottom = jnp.concatenate([jnp.where(first, zero, low), jnp.where(first, zero, high)], axis=1)
    return jnp.concatenate([top, bottom], axis=0)


def solve_windows(pa, pb, za, zb, pivots_row):
    alo, ahi = halves(pa, pb)
    zero = jnp.zeros((64, 64), jnp.float32)

    def block_rows(x, first):
        left = jnp.concatenate([x[:, :64], zero] if first else [zero, x[:, 64:]], axis=1)
        return left

    lo_a, lo_b = alo[:64], alo[64:]
    hi_a, hi_b = ahi[:64], ahi[64:]
    joint = jnp.concatenate(
        [
            jnp.concatenate([block_rows(lo_a, True), block_rows(hi_a, True)], axis=1),
            jnp.concatenate([block_rows(lo_a, False), block_rows(hi_a, False)], axis=1),
            jnp.concatenate([block_rows(lo_b, True), block_rows(hi_b, True)], axis=1),
            jnp.concatenate([block_rows(lo_b, False), block_rows(hi_b, False)], axis=1),
        ],
        axis=0,
    )
    low, high = lo_a, hi_a
    for sweep in range(2):
        if sweep:
            image = dot_nn(jnp.concatenate([low, high], axis=1), joint)
            low, high = image[:, :128], image[:, 128:]
        gram = dot_nt(jnp.concatenate([low, high], axis=1), masked_pair(low, high))
        low, high = whiten(gram, low, high)
    basis = jnp.concatenate([low, high], axis=1)
    image = dot_nn(basis, joint)
    prod = basis * image
    first = lax.broadcasted_iota(jnp.int32, (8, 256), 1) % 128 < 64
    row = lax.broadcasted_iota(jnp.int32, (8, 256), 0)
    pick = jnp.where((row == 0) & first, 1.0, 0.0) + jnp.where((row == 1) & (~first), 1.0, 0.0)
    squares = dot_nt(pick, prod)
    j = lax.broadcasted_iota(jnp.int32, (256, 128), 0)
    lane = lax.broadcasted_iota(jnp.int32, (256, 128), 1)
    own = (j // 64) % 2 == lane // 64
    dim = j % 64 + 64 * (j // 128)
    onehot = jnp.where(own & (dim == pivots_row), 1.0, 0.0)
    picked = dot_nn(basis, onehot)
    r = lax.broadcasted_iota(jnp.int32, (64, 128), 0)
    c = lax.broadcasted_iota(jnp.int32, (64, 128), 1)
    weight = jnp.sum(jnp.where(c % 64 == r, picked, 0.0), axis=0, keepdims=True) * math.sqrt(128)
    zlo, zhi = halves(za, zb)
    proj = dot_nt(jnp.concatenate([zlo, zhi], axis=1), masked_pair(low, high)) * weight
    return jnp.sqrt(squares[:2]), proj


MESH = pl.DeviceIdType.MESH
CHUNKS = 8


def rdma(src, dst, send, recv, where):
    return pltpu.make_async_remote_copy(
        src_ref=src, dst_ref=dst, send_sem=send, recv_sem=recv, device_id=where, device_id_type=MESH
    )


def gram_of(x):
    return lax.dot_general(
        x, x, (((0,), (0,)), ((), ())), precision=lax.Precision.HIGHEST, preferred_element_type=jnp.float32
    )


def sum_kernel(snap_hbm, sketch_hbm, own_ref, grams_ref,
               snap, sketch, part, rs_buf, ag_buf, gath, mate,
               in_sem, rs_send, rs_recv, ag_send, ag_recv, xy_send, xy_recv, mate_send, mate_recv):
    d = lax.axis_index("dof")
    w = lax.axis_index("win")
    nd, nw = 16, 16
    core = lax.rem(d, 2)
    partner = d + 1 - 2 * core
    depth = sketch.shape[1]
    gath[...] = jnp.zeros_like(gath)
    mate[...] = jnp.zeros_like(mate)
    barrier = pltpu.get_barrier_semaphore()
    for k in range(1, 16):
        pl.semaphore_signal(barrier, inc=1, device_id={"dof": lax.rem(d + k, nd)}, device_id_type=MESH)
        pl.semaphore_signal(barrier, inc=1, device_id={"win": lax.rem(w + k, nw)}, device_id_type=MESH)
    loads = []
    for i in range(CHUNKS):
        a = pltpu.make_async_copy(sketch_hbm.at[pl.ds(i * depth, depth), :], sketch.at[i], in_sem.at[0, i])
        b = pltpu.make_async_copy(snap_hbm.at[:, pl.ds(i * depth, depth)], snap.at[i], in_sem.at[1, i])
        a.start()
        b.start()
        loads.append((a, b))
    total = jnp.zeros((64, 128), jnp.float32)
    for i in range(CHUNKS):
        for copy in loads[i]:
            copy.wait()
        total = total + jnp.dot(snap[i], sketch[i], preferred_element_type=jnp.float32)
    for p in range(16):
        part[p] = total[4 * p : 4 * p + 4, :]
    pl.semaphore_wait(barrier, 30)
    order = [8, 9, 7, 6, 10, 5, 11, 4, 12, 3, 13, 2, 14, 15, 1]
    sends = []
    for k in order:
        q = lax.rem(d + k, nd)
        copy = rdma(part.at[q], rs_buf.at[d], rs_send.at[k], rs_recv.at[d], {"dof": q})
        copy.start()
        sends.append(copy)
    rs_buf[d] = part[d]
    for k in reversed(order):
        q = lax.rem(d + k, nd)
        rdma(part.at[q], rs_buf.at[q], rs_send.at[k], rs_recv.at[q], {"dof": q}).wait_recv()
    ag_buf[d] = jnp.sum(rs_buf[...], axis=0)
    for k in order:
        q = lax.rem(d + k, nd)
        copy = rdma(ag_buf.at[d], ag_buf.at[d], ag_send.at[k], ag_recv.at[d], {"dof": q})
        copy.start()
        sends.append(copy)
    forwards = []

    def forward(k, q):
        z = q // 2
        for v in range(1, 16):
            copy = rdma(ag_buf.at[q], gath.at[w, z], xy_send.at[k // 2, v], xy_recv.at[w, z], {"win": v})
            forwards.append((v, copy))

            @pl.when(v > w)
            def _():
                copy.start()

    forward(0, d)
    for k in reversed(order):
        q = lax.rem(d + k, nd)
        rdma(ag_buf.at[q], ag_buf.at[q], ag_send.at[k], ag_recv.at[q], {"dof": q}).wait_recv()
        if k % 2 == 0:
            forward(k, q)
    own = ag_buf[...].reshape(64, 128)
    own_ref[...] = own
    ma = gram_of(own[:32])
    mab = ma + gram_of(own[32:])
    for v in range(15):
        @pl.when(v < w)
        def _():
            for z in range(8):
                rdma(ag_buf.at[0], gath.at[v, z], xy_send.at[0, v], xy_recv.at[v, z], {"win": v}).wait_recv()
            rdma(gath.at[v], mate.at[v], mate_send.at[v], mate_recv.at[v], {"dof": partner}).start()
    base = gram_of(gath[...].reshape(512, 128))
    for v in range(15):
        @pl.when(v < w)
        def _():
            rdma(gath.at[v], mate.at[v], mate_send.at[v], mate_recv.at[v], {"dof": partner}).wait()
    base = base + gram_of(mate[...].reshape(512, 128))
    eye = jnp.where(
        lax.broadcasted_iota(jnp.int32, (128, 128), 0) == lax.broadcasted_iota(jnp.int32, (128, 128), 1), 1.0, 0.0
    )
    count = jnp.full((128, 128), 64 * w, jnp.int32).astype(jnp.float32)
    grams_ref[0] = eye + (base + ma) / (count + 32.0)
    grams_ref[1] = eye + (base + mab) / (count + 64.0)
    for copy in sends:
        copy.wait_send()
    for v, copy in forwards:
        @pl.when(v > w)
        def _():
            copy.wait_send()


def sum_call(snapshots, sketch_matrix, stop=4):
    depth = sketch_matrix.shape[0] // CHUNKS
    f32 = jnp.float32
    return pl.pallas_call(
        sum_kernel,
        out_shape=(jax.ShapeDtypeStruct((64, 128), f32), jax.ShapeDtypeStruct((2, 128, 128), f32)),
        in_specs=[pl.BlockSpec(memory_space=pltpu.HBM)] * 2,
        out_specs=(pl.BlockSpec(memory_space=pltpu.VMEM),) * 2,
        scratch_shapes=[
            pltpu.VMEM((CHUNKS, 64, depth), jnp.bfloat16),
            pltpu.VMEM((CHUNKS, depth, 128), jnp.bfloat16),
            pltpu.VMEM((16, 4, 128), f32),
            pltpu.VMEM((16, 4, 128), f32),
            pltpu.VMEM((16, 4, 128), f32),
            pltpu.VMEM((16, 8, 4, 128), f32),
            pltpu.VMEM((16, 8, 4, 128), f32),
            pltpu.SemaphoreType.DMA((2, CHUNKS)),
            pltpu.SemaphoreType.DMA((16,)),
            pltpu.SemaphoreType.DMA((16,)),
            pltpu.SemaphoreType.DMA((16,)),
            pltpu.SemaphoreType.DMA((16,)),
            pltpu.SemaphoreType.DMA((8, 16)),
            pltpu.SemaphoreType.DMA((16, 8)),
            pltpu.SemaphoreType.DMA((16,)),
            pltpu.SemaphoreType.DMA((16,)),
        ],
        compiler_params=pltpu.CompilerParams(collective_id=0, has_side_effects=True, vmem_limit_bytes=52 * 1024 * 1024),
    )(snapshots.T, sketch_matrix)

def solve_kernel(own_ref, grams_ref, pivots_ref, sing_ref, proj_ref):
    piv = pivots_ref[...]
    piv_row = jnp.concatenate([piv[0:1, :], piv[1:2, :]], axis=1)
    sing, proj = solve_windows(grams_ref[0], grams_ref[1], own_ref[:32, :], own_ref[32:, :], piv_row)
    sing_ref[...] = sing
    proj_ref[0] = proj[:, :64]
    proj_ref[1] = proj[:, 64:]


def local(snapshots, sketch_matrix, pivots):
    own, grams = sum_call(snapshots, sketch_matrix)
    sing, proj = pl.pallas_call(
        solve_kernel,
        out_shape=(jax.ShapeDtypeStruct((2, 64), jnp.float32), jax.ShapeDtypeStruct((2, 32, 64), jnp.float32)),
        in_specs=[pl.BlockSpec(memory_space=pltpu.VMEM)] * 3,
        out_specs=(pl.BlockSpec(memory_space=pltpu.VMEM),) * 2,
        compiler_params=pltpu.CompilerParams(vmem_limit_bytes=16 * 1024 * 1024),
    )(own, grams, pivots)
    return sing, jnp.swapaxes(proj, 1, 2)


def solution(mesh):
    placed = (P("dof", "win"), P("dof", None), P("win", None))
    return jax.shard_map(
        local,
        mesh=mesh,
        in_specs=placed,
        out_specs=(P("win", None), P("win", None, None)),
        check_vma=False,
    )
```

```python
import functools
import math

import jax
import jax.numpy as jnp
from jax import lax
from jax.experimental import pallas as pl
from jax.experimental.pallas import tpu as pltpu
from jax.sharding import PartitionSpec as P

HIGHEST_PREC = lax.Precision.HIGHEST
RANK = 64
NT = (((1,), (1,)), ((), ()))


def dot_nt(a, b):
    return lax.dot_general(a, b, NT, precision=HIGHEST_PREC, preferred_element_type=jnp.float32)


def dot_nn(a, b):
    return lax.dot_general(a, b, (((1,), (0,)), ((), ())), precision=HIGHEST_PREC, preferred_element_type=jnp.float32)


def halves(a, b):
    return jnp.concatenate([a[:, :64], b[:, :64]], axis=1), jnp.concatenate([a[:, 64:], b[:, 64:]], axis=1)


def split_rows(x):
    return [x[8 * i : 8 * i + 8, :] for i in range(8)]


def whiten(gram, low, high):
    lane = lax.broadcasted_iota(jnp.int32, (8, 128), 1)
    sub = lax.broadcasted_iota(jnp.int32, (8, 128), 0)
    base = lane - lane % 64
    v0, v1, v2 = split_rows(gram), split_rows(low), split_rows(high)
    for kb in range(8):
        cols = []
        for j in range(8):
            idx = base + (8 * kb + j)
            cols.append({i: jnp.take_along_axis(v0[i], idx, axis=1) for i in range(kb, 8)})
        diag = cols[0][kb]
        for p in range(8):
            pivot = jnp.broadcast_to(cols[p][kb][p : p + 1, :], (8, 128))
            if p:
                diag = jnp.where(sub >= p, pivot, diag)
            else:
                diag = pivot
            inv = 1.0 / pivot
            mult = {i: cols[p][i] * inv for i in range(kb, 8)}
            mult[kb] = jnp.where(sub > p, mult[kb], 0.0)
            for j in range(p + 1, 8):
                row = jnp.broadcast_to(cols[j][kb][p : p + 1, :], (8, 128))
                for i in range(kb, 8):
                    cols[j][i] = cols[j][i] - mult[i] * row
            for v in (v0, v1, v2) if kb < 7 else (v1, v2):
                row = jnp.broadcast_to(v[kb][p : p + 1, :], (8, 128))
                for i in range(kb, 8):
                    v[i] = v[i] - mult[i] * row
        scale = lax.rsqrt(diag)
        v1[kb] = v1[kb] * scale
        v2[kb] = v2[kb] * scale
    return jnp.concatenate(v1, axis=0), jnp.concatenate(v2, axis=0)


def masked_pair(low, high):
    first = lax.broadcasted_iota(jnp.int32, (64, 128), 1) < 64
    zero = jnp.zeros((64, 128), jnp.float32)
    top = jnp.concatenate([jnp.where(first, low, zero), jnp.where(first, high, zero)], axis=1)
    bottom = jnp.concatenate([jnp.where(first, zero, low), jnp.where(first, zero, high)], axis=1)
    return jnp.concatenate([top, bottom], axis=0)


def solve_windows(pa, pb, za, zb, pivots_row):
    alo, ahi = halves(pa, pb)
    zero = jnp.zeros((64, 64), jnp.float32)

    def block_rows(x, first):
        left = jnp.concatenate([x[:, :64], zero] if first else [zero, x[:, 64:]], axis=1)
        return left

    lo_a, lo_b = alo[:64], alo[64:]
    hi_a, hi_b = ahi[:64], ahi[64:]
    joint = jnp.concatenate(
        [
            jnp.concatenate([block_rows(lo_a, True), block_rows(hi_a, True)], axis=1),
            jnp.concatenate([block_rows(lo_a, False), block_rows(hi_a, False)], axis=1),
            jnp.concatenate([block_rows(lo_b, True), block_rows(hi_b, True)], axis=1),
            jnp.concatenate([block_rows(lo_b, False), block_rows(hi_b, False)], axis=1),
        ],
        axis=0,
    )
    low, high = lo_a, hi_a
    for sweep in range(2):
        if sweep:
            image = dot_nn(jnp.concatenate([low, high], axis=1), joint)
            low, high = image[:, :128], image[:, 128:]
        gram = dot_nt(jnp.concatenate([low, high], axis=1), masked_pair(low, high))
        low, high = whiten(gram, low, high)
    basis = jnp.concatenate([low, high], axis=1)
    image = dot_nn(basis, joint)
    prod = basis * image
    first = lax.broadcasted_iota(jnp.int32, (8, 256), 1) % 128 < 64
    row = lax.broadcasted_iota(jnp.int32, (8, 256), 0)
    pick = jnp.where((row == 0) & first, 1.0, 0.0) + jnp.where((row == 1) & (~first), 1.0, 0.0)
    squares = dot_nt(pick, prod)
    j = lax.broadcasted_iota(jnp.int32, (256, 128), 0)
    lane = lax.broadcasted_iota(jnp.int32, (256, 128), 1)
    own = (j // 64) % 2 == lane // 64
    dim = j % 64 + 64 * (j // 128)
    onehot = jnp.where(own & (dim == pivots_row), 1.0, 0.0)
    picked = dot_nn(basis, onehot)
    r = lax.broadcasted_iota(jnp.int32, (64, 128), 0)
    c = lax.broadcasted_iota(jnp.int32, (64, 128), 1)
    weight = jnp.sum(jnp.where(c % 64 == r, picked, 0.0), axis=0, keepdims=True) * math.sqrt(128)
    zlo, zhi = halves(za, zb)
    proj = dot_nt(jnp.concatenate([zlo, zhi], axis=1), masked_pair(low, high)) * weight
    return jnp.sqrt(squares[:2]), proj


MESH = pl.DeviceIdType.MESH
CHUNKS = 8


def rdma(src, dst, send, recv, where):
    return pltpu.make_async_remote_copy(
        src_ref=src, dst_ref=dst, send_sem=send, recv_sem=recv, device_id=where, device_id_type=MESH
    )


def gram_of(x):
    return lax.dot_general(
        x, x, (((0,), (0,)), ((), ())), precision=lax.Precision.HIGHEST, preferred_element_type=jnp.float32
    )


def sum_kernel(snap_hbm, sketch_hbm, own_ref, grams_ref,
               snap, sketch, part, rs_buf, ag_buf, gath, gram_send, gram_recv,
               in_sem, rs_send, rs_recv, ag_send, ag_recv, ag_other, xy_send, xy_recv, pair_sem):
    d = lax.axis_index("dof")
    w = lax.axis_index("win")
    nd, nw = 16, 16
    core = lax.rem(d, 2)
    partner = d + 1 - 2 * core
    depth = sketch.shape[1]
    gath[...] = jnp.zeros_like(gath)
    barrier = pltpu.get_barrier_semaphore()
    for k in range(1, 16):
        pl.semaphore_signal(barrier, inc=1, device_id={"dof": lax.rem(d + k, nd)}, device_id_type=MESH)
        pl.semaphore_signal(barrier, inc=1, device_id={"win": lax.rem(w + k, nw)}, device_id_type=MESH)
    loads = []
    for i in range(CHUNKS):
        a = pltpu.make_async_copy(sketch_hbm.at[pl.ds(i * depth, depth), :], sketch.at[i], in_sem.at[0, i])
        b = pltpu.make_async_copy(snap_hbm.at[:, pl.ds(i * depth, depth)], snap.at[i], in_sem.at[1, i])
        a.start()
        b.start()
        loads.append((a, b))
    total = jnp.zeros((64, 128), jnp.float32)
    for i in range(CHUNKS):
        for copy in loads[i]:
            copy.wait()
        total = total + jnp.dot(snap[i], sketch[i], preferred_element_type=jnp.float32)
    for p in range(16):
        part[p] = total[4 * p : 4 * p + 4, :]
    pl.semaphore_wait(barrier, 30)
    order = [8, 9, 7, 6, 10, 5, 11, 4, 12, 3, 13, 2, 14, 15, 1]
    for k in order:
        q = lax.rem(d + k, nd)
        rdma(part.at[q], rs_buf.at[d], rs_send, rs_recv, {"dof": q}).start()
    rs_buf[d] = part[d]
    fifteen = pl.ds(0, 15)
    rdma(part.at[fifteen], rs_buf.at[fifteen], rs_send, rs_recv, {"dof": partner}).wait_recv()
    ag_buf[d] = jnp.sum(rs_buf[...], axis=0)
    z_here = d // 2
    for k in order:
        q = lax.rem(d + k, nd)
        arrival = ag_other if k % 2 else ag_recv.at[z_here]
        rdma(ag_buf.at[d], ag_buf.at[d], ag_send, arrival, {"dof": q}).start()

    def forward(q):
        z = q // 2
        for v in range(1, 16):
            @pl.when(v > w)
            def _():
                rdma(ag_buf.at[q], gath.at[w, z], xy_send.at[v], xy_recv.at[w], {"win": v}).start()

    forward(d)
    for k in reversed(order):
        if k % 2 == 0:
            q = lax.rem(d + k, nd)
            rdma(ag_buf.at[q], ag_buf.at[q], ag_send, ag_recv.at[q // 2], {"dof": q}).wait_recv()
            forward(q)
    eight = pl.ds(0, 8)
    rdma(ag_buf.at[eight], ag_buf.at[eight], ag_send, ag_other, {"dof": partner}).wait_recv()
    own = ag_buf[...].reshape(64, 128)
    own_ref[...] = own
    ma = gram_of(own[:32])
    mab = ma + gram_of(own[32:])
    for v in range(15):
        @pl.when(v < w)
        def _():
            rdma(gath.at[v], gath.at[v], xy_send.at[v], xy_recv.at[v], {"win": v}).wait_recv()
    gram_send[...] = gram_of(gath[...].reshape(512, 128))
    swap = rdma(gram_send, gram_recv, pair_sem.at[0], pair_sem.at[1], {"dof": partner})
    swap.start()
    rdma(part.at[fifteen], rs_buf.at[fifteen], rs_send, rs_recv, {"dof": partner}).wait_send()
    rdma(ag_buf.at[fifteen], ag_buf.at[fifteen], ag_send, ag_other, {"dof": partner}).wait_send()
    for v in range(1, 16):
        @pl.when(v > w)
        def _():
            rdma(ag_buf.at[eight], gath.at[w], xy_send.at[v], xy_recv.at[v], {"win": v}).wait_send()
    eye = jnp.where(
        lax.broadcasted_iota(jnp.int32, (128, 128), 0) == lax.broadcasted_iota(jnp.int32, (128, 128), 1), 1.0, 0.0
    )
    count = jnp.full((128, 128), 64 * w, jnp.int32).astype(jnp.float32)
    swap.wait()
    base = gram_send[...] + gram_recv[...]
    grams_ref[0] = eye + (base + ma) / (count + 32.0)
    grams_ref[1] = eye + (base + mab) / (count + 64.0)


def sum_call(snapshots, sketch_matrix, stop=4):
    depth = sketch_matrix.shape[0] // CHUNKS
    f32 = jnp.float32
    return pl.pallas_call(
        sum_kernel,
        out_shape=(jax.ShapeDtypeStruct((64, 128), f32), jax.ShapeDtypeStruct((2, 128, 128), f32)),
        in_specs=[pl.BlockSpec(memory_space=pl.ANY)] * 2,
        out_specs=(pl.BlockSpec(memory_space=pltpu.VMEM),) * 2,
        scratch_shapes=[
            pltpu.VMEM((CHUNKS, 64, depth), jnp.bfloat16),
            pltpu.VMEM((CHUNKS, depth, 128), jnp.bfloat16),
            pltpu.VMEM((16, 4, 128), f32),
            pltpu.VMEM((16, 4, 128), f32),
            pltpu.VMEM((16, 4, 128), f32),
            pltpu.VMEM((16, 8, 4, 128), f32),
            pltpu.VMEM((128, 128), f32),
            pltpu.VMEM((128, 128), f32),
            pltpu.SemaphoreType.DMA((2, CHUNKS)),
            pltpu.SemaphoreType.DMA,
            pltpu.SemaphoreType.DMA,
            pltpu.SemaphoreType.DMA,
            pltpu.SemaphoreType.DMA((8,)),
            pltpu.SemaphoreType.DMA,
            pltpu.SemaphoreType.DMA((16,)),
            pltpu.SemaphoreType.DMA((15,)),
            pltpu.SemaphoreType.DMA((2,)),
        ],
        compiler_params=pltpu.CompilerParams(collective_id=0, has_side_effects=True, vmem_limit_bytes=52 * 1024 * 1024),
    )(snapshots.T, sketch_matrix)

def solve_kernel(own_ref, grams_ref, pivots_ref, sing_ref, proj_ref):
    piv = pivots_ref[...]
    piv_row = jnp.concatenate([piv[0:1, :], piv[1:2, :]], axis=1)
    sing, proj = solve_windows(grams_ref[0], grams_ref[1], own_ref[:32, :], own_ref[32:, :], piv_row)
    sing_ref[...] = sing
    proj_ref[0] = proj[:, :64]
    proj_ref[1] = proj[:, 64:]


def local(snapshots, sketch_matrix, pivots):
    own, grams = sum_call(snapshots, sketch_matrix)
    sing, proj = pl.pallas_call(
        solve_kernel,
        out_shape=(jax.ShapeDtypeStruct((2, 64), jnp.float32), jax.ShapeDtypeStruct((2, 32, 64), jnp.float32)),
        in_specs=[pl.BlockSpec(memory_space=pltpu.VMEM)] * 3,
        out_specs=(pl.BlockSpec(memory_space=pltpu.VMEM),) * 2,
        compiler_params=pltpu.CompilerParams(vmem_limit_bytes=16 * 1024 * 1024),
    )(own, grams, pivots)
    return sing, jnp.swapaxes(proj, 1, 2)


def solution(mesh):
    placed = (P("dof", "win"), P("dof", None), P("win", None))
    return jax.shard_map(
        local,
        mesh=mesh,
        in_specs=placed,
        out_specs=(P("win", None), P("win", None, None)),
        check_vma=False,
    )
```

```python
import functools
import math

import jax
import jax.numpy as jnp
from jax import lax
from jax.experimental import pallas as pl
from jax.experimental.pallas import tpu as pltpu
from jax.sharding import PartitionSpec as P

HIGHEST_PREC = lax.Precision.HIGHEST
RANK = 64
NT = (((1,), (1,)), ((), ()))


def dot_nt(a, b):
    return lax.dot_general(a, b, NT, precision=HIGHEST_PREC, preferred_element_type=jnp.float32)


def dot_nn(a, b):
    return lax.dot_general(a, b, (((1,), (0,)), ((), ())), precision=HIGHEST_PREC, preferred_element_type=jnp.float32)


def halves(a, b):
    return jnp.concatenate([a[:, :64], b[:, :64]], axis=1), jnp.concatenate([a[:, 64:], b[:, 64:]], axis=1)


def split_rows(x):
    return [x[8 * i : 8 * i + 8, :] for i in range(8)]


def whiten(gram, low, high):
    lane = lax.broadcasted_iota(jnp.int32, (8, 128), 1)
    sub = lax.broadcasted_iota(jnp.int32, (8, 128), 0)
    base = lane - lane % 64
    v0, v1, v2 = split_rows(gram * 2.0**-32), split_rows(low), split_rows(high)

    def bcast(x, p):
        return jnp.broadcast_to(x[p : p + 1, :], (8, 128))

    for kb in range(8):
        cols = []
        for j in range(8):
            idx = base + (8 * kb + j)
            cols.append({i: jnp.take_along_axis(v0[i], idx, axis=1) for i in range(kb, 8)})
        diag = None
        for p in range(0, 8, 2):
            q = p + 1
            cp, cq = cols[p], cols[q]
            a, b, c = bcast(cp[kb], p), bcast(cp[kb], q), bcast(cq[kb], q)
            det = a * c - b * b
            inv = 1.0 / det
            inv_a = 1.0 / a
            m1, m2 = {}, {}
            for i in range(kb, 8):
                n1 = cp[i] * c - cq[i] * b
                n2 = cq[i] * a - cp[i] * b
                if i == kb:
                    n1 = jnp.where(sub > q, n1, 0.0)
                    n2 = jnp.where(sub > q, n2, 0.0)
                m1[i], m2[i] = n1 * inv, n2 * inv
            m1[kb] = jnp.where(sub == q, b * inv_a, m1[kb])
            dq = det * inv_a
            diag = a if diag is None else jnp.where(sub >= p, a, diag)
            diag = jnp.where(sub >= q, dq, diag)
            for j in range(q + 1, 8):
                rp, rq = bcast(cols[j][kb], p), bcast(cols[j][kb], q)
                for i in range(kb, 8):
                    cols[j][i] = cols[j][i] - (m1[i] * rp + m2[i] * rq)
            for v in (v0, v1, v2) if kb < 7 else (v1, v2):
                rp, rq = bcast(v[kb], p), bcast(v[kb], q)
                for i in range(kb, 8):
                    v[i] = v[i] - (m1[i] * rp + m2[i] * rq)
        scale = lax.rsqrt(diag) * 2.0**-16
        v1[kb] = v1[kb] * scale
        v2[kb] = v2[kb] * scale
    return jnp.concatenate(v1, axis=0), jnp.concatenate(v2, axis=0)


def masked_pair(low, high):
    first = lax.broadcasted_iota(jnp.int32, (64, 128), 1) < 64
    zero = jnp.zeros((64, 128), jnp.float32)
    top = jnp.concatenate([jnp.where(first, low, zero), jnp.where(first, high, zero)], axis=1)
    bottom = jnp.concatenate([jnp.where(first, zero, low), jnp.where(first, zero, high)], axis=1)
    return jnp.concatenate([top, bottom], axis=0)


def solve_windows(pa, pb, za, zb, pivots_row):
    alo, ahi = halves(pa, pb)
    zero = jnp.zeros((64, 64), jnp.float32)

    def block_rows(x, first):
        left = jnp.concatenate([x[:, :64], zero] if first else [zero, x[:, 64:]], axis=1)
        return left

    lo_a, lo_b = alo[:64], alo[64:]
    hi_a, hi_b = ahi[:64], ahi[64:]
    joint = jnp.concatenate(
        [
            jnp.concatenate([block_rows(lo_a, True), block_rows(hi_a, True)], axis=1),
            jnp.concatenate([block_rows(lo_a, False), block_rows(hi_a, False)], axis=1),
            jnp.concatenate([block_rows(lo_b, True), block_rows(hi_b, True)], axis=1),
            jnp.concatenate([block_rows(lo_b, False), block_rows(hi_b, False)], axis=1),
        ],
        axis=0,
    )
    low, high = lo_a, hi_a
    for sweep in range(2):
        if sweep:
            image = dot_nn(jnp.concatenate([low, high], axis=1), joint)
            low, high = image[:, :128], image[:, 128:]
        gram = dot_nt(jnp.concatenate([low, high], axis=1), masked_pair(low, high))
        low, high = whiten(gram, low, high)
    basis = jnp.concatenate([low, high], axis=1)
    image = dot_nn(basis, joint)
    prod = basis * image
    first = lax.broadcasted_iota(jnp.int32, (8, 256), 1) % 128 < 64
    row = lax.broadcasted_iota(jnp.int32, (8, 256), 0)
    pick = jnp.where((row == 0) & first, 1.0, 0.0) + jnp.where((row == 1) & (~first), 1.0, 0.0)
    squares = dot_nt(pick, prod)
    j = lax.broadcasted_iota(jnp.int32, (256, 128), 0)
    lane = lax.broadcasted_iota(jnp.int32, (256, 128), 1)
    own = (j // 64) % 2 == lane // 64
    dim = j % 64 + 64 * (j // 128)
    onehot = jnp.where(own & (dim == pivots_row), 1.0, 0.0)
    picked = dot_nn(basis, onehot)
    r = lax.broadcasted_iota(jnp.int32, (64, 128), 0)
    c = lax.broadcasted_iota(jnp.int32, (64, 128), 1)
    weight = jnp.sum(jnp.where(c % 64 == r, picked, 0.0), axis=0, keepdims=True) * math.sqrt(128)
    zlo, zhi = halves(za, zb)
    proj = dot_nt(jnp.concatenate([zlo, zhi], axis=1), masked_pair(low, high)) * weight
    return jnp.sqrt(squares[:2]), proj


MESH = pl.DeviceIdType.MESH
CHUNKS = 8


def rdma(src, dst, send, recv, where):
    return pltpu.make_async_remote_copy(
        src_ref=src, dst_ref=dst, send_sem=send, recv_sem=recv, device_id=where, device_id_type=MESH
    )


def gram_of(x):
    return lax.dot_general(
        x, x, (((0,), (0,)), ((), ())), precision=lax.Precision.HIGHEST, preferred_element_type=jnp.float32
    )


def gram_split(x):
    high = x.astype(jnp.bfloat16)
    low = (x - high.astype(jnp.float32)).astype(jnp.bfloat16)
    both = jnp.concatenate([high, low], axis=1)
    g = lax.dot_general(both, both, (((0,), (0,)), ((), ())), preferred_element_type=jnp.float32)
    return (g[:128, :128] + g[128:, 128:]) + (g[:128, 128:] + g[128:, :128])


def slot_of(q):
    return lax.rem(q, 2) * 8 + q // 2


def sum_kernel(snap_hbm, sketch_hbm, own_ref, grams_ref,
               snap, sketch, part, rs_buf, ag_buf, gath, gram_send, gram_recv,
               in_sem, rs_send, rs_recv, ag_send, ag_recv, ag_other, xy_send, xy_recv, pair_sem):
    d = lax.axis_index("dof")
    w = lax.axis_index("win")
    nd, nw = 16, 16
    core = lax.rem(d, 2)
    partner = d + 1 - 2 * core
    depth = sketch.shape[1]
    gath[...] = jnp.zeros_like(gath)
    barrier = pltpu.get_barrier_semaphore()
    for k in range(1, 16):
        pl.semaphore_signal(barrier, inc=1, device_id={"dof": lax.rem(d + k, nd)}, device_id_type=MESH)
        pl.semaphore_signal(barrier, inc=1, device_id={"win": lax.rem(w + k, nw)}, device_id_type=MESH)
    loads = []
    for i in range(CHUNKS):
        a = pltpu.make_async_copy(sketch_hbm.at[pl.ds(i * depth, depth), :], sketch.at[i], in_sem.at[0, i])
        b = pltpu.make_async_copy(snap_hbm.at[:, pl.ds(i * depth, depth)], snap.at[i], in_sem.at[1, i])
        a.start()
        b.start()
        loads.append((a, b))
    total = jnp.zeros((64, 128), jnp.float32)
    for i in range(CHUNKS):
        for copy in loads[i]:
            copy.wait()
        total = total + jnp.dot(snap[i], sketch[i], preferred_element_type=jnp.float32)
    for p in range(16):
        part[p] = total[4 * p : 4 * p + 4, :]
    pl.semaphore_wait(barrier, 30)
    me = slot_of(d)
    order = [8, 9, 7, 6, 10, 5, 11, 4, 12, 3, 13, 2, 14, 15, 1]
    for k in order:
        q = lax.rem(d + k, nd)
        rdma(part.at[slot_of(q)], rs_buf.at[me], rs_send, rs_recv, {"dof": q}).start()
    rs_buf[me] = part[me]
    fifteen = pl.ds(0, 15)
    rdma(part.at[fifteen], rs_buf.at[fifteen], rs_send, rs_recv, {"dof": partner}).wait_recv()
    ag_buf[me] = jnp.sum(rs_buf[...], axis=0)
    z_here = d // 2
    for k in order:
        q = lax.rem(d + k, nd)
        arrival = ag_other if k % 2 else ag_recv.at[z_here]
        rdma(ag_buf.at[me], ag_buf.at[me], ag_send, arrival, {"dof": q}).start()

    def wait_piece(q):
        rdma(ag_buf.at[slot_of(q)], ag_buf.at[slot_of(q)], ag_send, ag_recv.at[q // 2], {"dof": q}).wait_recv()

    def forward(first, count):
        src = ag_buf.at[pl.ds(core * 8 + first, count)]
        dst = gath.at[w, pl.ds(first, count)]

        def send(v, carry):
            rdma(src, dst, xy_send.at[v], xy_recv.at[w], {"win": v}).start()
            return carry

        lax.fori_loop(w + 1, 16, send, 0)

    forward(z_here, 1)
    for k in reversed(order):
        if k % 2 == 0:
            q = lax.rem(d + k, nd)
            wait_piece(q)
            forward(q // 2, 1)
    eight = pl.ds(0, 8)
    rdma(ag_buf.at[eight], ag_buf.at[eight], ag_send, ag_other, {"dof": partner}).wait_recv()
    own = ag_buf[...].reshape(64, 128)
    own_ref[...] = own
    ma = gram_of(own[:32])
    mab = ma + gram_of(own[32:])
    for v in range(15):
        @pl.when(v < w)
        def _():
            rdma(gath.at[v], gath.at[v], xy_send.at[v], xy_recv.at[v], {"win": v}).wait_recv()
    gram_send[...] = gram_split(gath[...].reshape(512, 128))
    swap = rdma(gram_send, gram_recv, pair_sem.at[0], pair_sem.at[1], {"dof": partner})
    swap.start()
    rdma(part.at[fifteen], rs_buf.at[fifteen], rs_send, rs_recv, {"dof": partner}).wait_send()
    rdma(ag_buf.at[fifteen], ag_buf.at[fifteen], ag_send, ag_other, {"dof": partner}).wait_send()
    for v in range(1, 16):
        @pl.when(v > w)
        def _():
            rdma(ag_buf.at[eight], gath.at[w], xy_send.at[v], xy_recv.at[v], {"win": v}).wait_send()
    eye = jnp.where(
        lax.broadcasted_iota(jnp.int32, (128, 128), 0) == lax.broadcasted_iota(jnp.int32, (128, 128), 1), 1.0, 0.0
    )
    count = jnp.full((128, 128), 64 * w, jnp.int32).astype(jnp.float32)
    swap.wait()
    base = gram_send[...] + gram_recv[...]
    grams_ref[0] = eye + (base + ma) / (count + 32.0)
    grams_ref[1] = eye + (base + mab) / (count + 64.0)


def sum_call(snapshots, sketch_matrix):
    depth = sketch_matrix.shape[0] // CHUNKS
    f32 = jnp.float32
    return pl.pallas_call(
        sum_kernel,
        out_shape=(jax.ShapeDtypeStruct((64, 128), f32), jax.ShapeDtypeStruct((2, 128, 128), f32)),
        in_specs=[pl.BlockSpec(memory_space=pl.ANY)] * 2,
        out_specs=(pl.BlockSpec(memory_space=pltpu.VMEM),) * 2,
        scratch_shapes=[
            pltpu.VMEM((CHUNKS, 64, depth), jnp.bfloat16),
            pltpu.VMEM((CHUNKS, depth, 128), jnp.bfloat16),
            pltpu.VMEM((16, 4, 128), f32),
            pltpu.VMEM((16, 4, 128), f32),
            pltpu.VMEM((16, 4, 128), f32),
            pltpu.VMEM((16, 8, 4, 128), f32),
            pltpu.VMEM((128, 128), f32),
            pltpu.VMEM((128, 128), f32),
            pltpu.SemaphoreType.DMA((2, CHUNKS)),
            pltpu.SemaphoreType.DMA,
            pltpu.SemaphoreType.DMA,
            pltpu.SemaphoreType.DMA,
            pltpu.SemaphoreType.DMA((8,)),
            pltpu.SemaphoreType.DMA,
            pltpu.SemaphoreType.DMA((16,)),
            pltpu.SemaphoreType.DMA((16,)),
            pltpu.SemaphoreType.DMA((2,)),
        ],
        compiler_params=pltpu.CompilerParams(collective_id=0, has_side_effects=True, vmem_limit_bytes=52 * 1024 * 1024),
    )(snapshots.T, sketch_matrix)

def solve_kernel(own_ref, grams_ref, pivots_ref, sing_ref, proj_ref):
    piv = pivots_ref[...]
    piv_row = jnp.concatenate([piv[0:1, :], piv[1:2, :]], axis=1)
    sing, proj = solve_windows(grams_ref[0], grams_ref[1], own_ref[:32, :], own_ref[32:, :], piv_row)
    sing_ref[...] = sing
    proj_ref[0] = proj[:, :64]
    proj_ref[1] = proj[:, 64:]


def local(snapshots, sketch_matrix, pivots):
    own, grams = sum_call(snapshots, sketch_matrix)
    sing, proj = pl.pallas_call(
        solve_kernel,
        out_shape=(jax.ShapeDtypeStruct((2, 64), jnp.float32), jax.ShapeDtypeStruct((2, 32, 64), jnp.float32)),
        in_specs=[pl.BlockSpec(memory_space=pltpu.VMEM)] * 3,
        out_specs=(pl.BlockSpec(memory_space=pltpu.VMEM),) * 2,
        compiler_params=pltpu.CompilerParams(vmem_limit_bytes=16 * 1024 * 1024),
    )(own, grams, pivots)
    return sing, jnp.swapaxes(proj, 1, 2)


def solution(mesh):
    placed = (P("dof", "win"), P("dof", None), P("win", None))
    return jax.shard_map(
        local,
        mesh=mesh,
        in_specs=placed,
        out_specs=(P("win", None), P("win", None, None)),
        check_vma=False,
    )
```

```python
import functools
import math

import jax
import jax.numpy as jnp
from jax import lax
from jax.experimental import pallas as pl
from jax.experimental.pallas import tpu as pltpu
from jax.sharding import PartitionSpec as P

HIGHEST_PREC = lax.Precision.HIGHEST
RANK = 64
NT = (((1,), (1,)), ((), ()))


def dot_nt(a, b):
    return lax.dot_general(a, b, NT, precision=HIGHEST_PREC, preferred_element_type=jnp.float32)


def dot_nn(a, b):
    return lax.dot_general(a, b, (((1,), (0,)), ((), ())), precision=HIGHEST_PREC, preferred_element_type=jnp.float32)


def halves(a, b):
    return jnp.concatenate([a[:, :64], b[:, :64]], axis=1), jnp.concatenate([a[:, 64:], b[:, 64:]], axis=1)


def split_rows(x):
    return [x[8 * i : 8 * i + 8, :] for i in range(8)]


def whiten(gram, *payload):
    lane = lax.broadcasted_iota(jnp.int32, (8, 128), 1)
    sub = lax.broadcasted_iota(jnp.int32, (8, 128), 0)
    base = lane - lane % 64
    small = 2.0**-32
    if gram is None:
        rows = [split_rows(x * small) for x in payload]
        pivots_from, unit = rows[0], 2.0**16
    else:
        rows = [split_rows(x) for x in payload]
        pivots_from, unit = split_rows(gram * small), 2.0**-16

    def bcast(x, p):
        return jnp.broadcast_to(x[p : p + 1, :], (8, 128))

    for kb in range(8):
        cols = []
        for j in range(8):
            idx = base + (8 * kb + j)
            cols.append({i: jnp.take_along_axis(pivots_from[i], idx, axis=1) for i in range(kb, 8)})
        diag = None
        for p in range(0, 8, 2):
            q = p + 1
            cp, cq = cols[p], cols[q]
            a, b, c = bcast(cp[kb], p), bcast(cp[kb], q), bcast(cq[kb], q)
            det = a * c - b * b
            inv = 1.0 / det
            inv_a = 1.0 / a
            m1, m2 = {}, {}
            for i in range(kb, 8):
                n1 = cp[i] * c - cq[i] * b
                n2 = cq[i] * a - cp[i] * b
                if i == kb:
                    n1 = jnp.where(sub > q, n1, 0.0)
                    n2 = jnp.where(sub > q, n2, 0.0)
                m1[i], m2[i] = n1 * inv, n2 * inv
            m1[kb] = jnp.where(sub == q, b * inv_a, m1[kb])
            dq = det * inv_a
            diag = a if diag is None else jnp.where(sub >= p, a, diag)
            diag = jnp.where(sub >= q, dq, diag)
            for j in range(q + 1, 8):
                rp, rq = bcast(cols[j][kb], p), bcast(cols[j][kb], q)
                for i in range(kb, 8):
                    cols[j][i] = cols[j][i] - (m1[i] * rp + m2[i] * rq)
            for v in rows if gram is None or kb == 7 else [pivots_from] + rows:
                rp, rq = bcast(v[kb], p), bcast(v[kb], q)
                for i in range(kb, 8):
                    v[i] = v[i] - (m1[i] * rp + m2[i] * rq)
        scale = lax.rsqrt(diag) * unit
        for v in rows:
            v[kb] = v[kb] * scale
    return [jnp.concatenate(v, axis=0) for v in rows]


def masked_pair(low, high):
    first = lax.broadcasted_iota(jnp.int32, (64, 128), 1) < 64
    zero = jnp.zeros((64, 128), jnp.float32)
    top = jnp.concatenate([jnp.where(first, low, zero), jnp.where(first, high, zero)], axis=1)
    bottom = jnp.concatenate([jnp.where(first, zero, low), jnp.where(first, zero, high)], axis=1)
    return jnp.concatenate([top, bottom], axis=0)


def solve_windows(pa, pb, za, zb, pivots_row):
    alo, ahi = halves(pa, pb)
    zero = jnp.zeros((64, 64), jnp.float32)

    def block_rows(x, first):
        left = jnp.concatenate([x[:, :64], zero] if first else [zero, x[:, 64:]], axis=1)
        return left

    lo_a, lo_b = alo[:64], alo[64:]
    hi_a, hi_b = ahi[:64], ahi[64:]
    joint = jnp.concatenate(
        [
            jnp.concatenate([block_rows(lo_a, True), block_rows(hi_a, True)], axis=1),
            jnp.concatenate([block_rows(lo_a, False), block_rows(hi_a, False)], axis=1),
            jnp.concatenate([block_rows(lo_b, True), block_rows(hi_b, True)], axis=1),
            jnp.concatenate([block_rows(lo_b, False), block_rows(hi_b, False)], axis=1),
        ],
        axis=0,
    )
    square = dot_nn(jnp.concatenate([lo_a, hi_a], axis=1), joint)
    low, high = whiten(None, square[:, :128], square[:, 128:])
    gram = dot_nt(jnp.concatenate([low, high], axis=1), masked_pair(low, high))
    low, high = whiten(gram, low, high)
    basis = jnp.concatenate([low, high], axis=1)
    image = dot_nn(basis, joint)
    prod = basis * image
    first = lax.broadcasted_iota(jnp.int32, (8, 256), 1) % 128 < 64
    row = lax.broadcasted_iota(jnp.int32, (8, 256), 0)
    pick = jnp.where((row == 0) & first, 1.0, 0.0) + jnp.where((row == 1) & (~first), 1.0, 0.0)
    squares = dot_nt(pick, prod)
    j = lax.broadcasted_iota(jnp.int32, (256, 128), 0)
    lane = lax.broadcasted_iota(jnp.int32, (256, 128), 1)
    own = (j // 64) % 2 == lane // 64
    dim = j % 64 + 64 * (j // 128)
    onehot = jnp.where(own & (dim == pivots_row), 1.0, 0.0)
    picked = dot_nn(basis, onehot)
    r = lax.broadcasted_iota(jnp.int32, (64, 128), 0)
    c = lax.broadcasted_iota(jnp.int32, (64, 128), 1)
    weight = jnp.sum(jnp.where(c % 64 == r, picked, 0.0), axis=0, keepdims=True) * math.sqrt(128)
    zlo, zhi = halves(za, zb)
    proj = dot_nt(jnp.concatenate([zlo, zhi], axis=1), masked_pair(low, high)) * weight
    return jnp.sqrt(squares[:2]), proj


MESH = pl.DeviceIdType.MESH
CHUNKS = 8


def rdma(src, dst, send, recv, where):
    return pltpu.make_async_remote_copy(
        src_ref=src, dst_ref=dst, send_sem=send, recv_sem=recv, device_id=where, device_id_type=MESH
    )


def gram_of(x):
    return lax.dot_general(
        x, x, (((0,), (0,)), ((), ())), precision=lax.Precision.HIGHEST, preferred_element_type=jnp.float32
    )


def gram_split(x):
    high = x.astype(jnp.bfloat16)
    low = (x - high.astype(jnp.float32)).astype(jnp.bfloat16)
    both = jnp.concatenate([high, low], axis=1)
    g = lax.dot_general(both, both, (((0,), (0,)), ((), ())), preferred_element_type=jnp.float32)
    return (g[:128, :128] + g[128:, 128:]) + (g[:128, 128:] + g[128:, :128])


def slot_of(q):
    return lax.rem(q, 2) * 8 + q // 2


def sum_kernel(snap_hbm, sketch_hbm, own_ref, grams_ref,
               snap, sketch, part, rs_buf, ag_buf, gath, gram_send, gram_recv,
               in_sem, rs_send, rs_recv, ag_send, ag_recv, ag_other, xy_send, xy_recv, pair_sem):
    d = lax.axis_index("dof")
    w = lax.axis_index("win")
    nd, nw = 16, 16
    core = lax.rem(d, 2)
    partner = d + 1 - 2 * core
    depth = sketch.shape[1]
    loads = []
    for i in range(CHUNKS):
        a = pltpu.make_async_copy(sketch_hbm.at[pl.ds(i * depth, depth), :], sketch.at[i], in_sem.at[0, i])
        b = pltpu.make_async_copy(snap_hbm.at[:, pl.ds(i * depth, depth)], snap.at[i], in_sem.at[1, i])
        a.start()
        b.start()
        loads.append((a, b))
    gath[...] = jnp.zeros_like(gath)
    barrier = pltpu.get_barrier_semaphore()
    for k in range(1, 16):
        pl.semaphore_signal(barrier, inc=1, device_id={"dof": lax.rem(d + k, nd)}, device_id_type=MESH)
        pl.semaphore_signal(barrier, inc=1, device_id={"win": lax.rem(w + k, nw)}, device_id_type=MESH)
    total = jnp.zeros((64, 128), jnp.float32)
    for i in range(CHUNKS):
        for copy in loads[i]:
            copy.wait()
        total = total + jnp.dot(snap[i], sketch[i], preferred_element_type=jnp.float32)
    for p in range(16):
        part[p] = total[4 * p : 4 * p + 4, :]
    pl.semaphore_wait(barrier, 30)
    me = slot_of(d)
    order = [8, 9, 7, 6, 10, 5, 11, 4, 12, 3, 13, 2, 14, 15, 1]
    for k in order:
        q = lax.rem(d + k, nd)
        rdma(part.at[slot_of(q)], rs_buf.at[me], rs_send, rs_recv, {"dof": q}).start()
    rs_buf[me] = part[me]
    fifteen = pl.ds(0, 15)
    rdma(part.at[fifteen], rs_buf.at[fifteen], rs_send, rs_recv, {"dof": partner}).wait_recv()
    ag_buf[me] = jnp.sum(rs_buf[...], axis=0)
    z_here = d // 2
    for k in order:
        q = lax.rem(d + k, nd)
        arrival = ag_other if k % 2 else ag_recv.at[z_here]
        rdma(ag_buf.at[me], ag_buf.at[me], ag_send, arrival, {"dof": q}).start()

    def wait_piece(q):
        rdma(ag_buf.at[slot_of(q)], ag_buf.at[slot_of(q)], ag_send, ag_recv.at[q // 2], {"dof": q}).wait_recv()

    def forward(first, count):
        src = ag_buf.at[pl.ds(core * 8 + first, count)]
        dst = gath.at[w, pl.ds(first, count)]

        def send(v, carry):
            rdma(src, dst, xy_send.at[v], xy_recv.at[w], {"win": v}).start()
            return carry

        lax.fori_loop(w + 1, 16, send, 0)

    forward(z_here, 1)
    for k in reversed(order):
        if k % 2 == 0:
            q = lax.rem(d + k, nd)
            wait_piece(q)
            forward(q // 2, 1)
    eight = pl.ds(0, 8)
    rdma(ag_buf.at[eight], ag_buf.at[eight], ag_send, ag_other, {"dof": partner}).wait_recv()
    own = ag_buf[...].reshape(64, 128)
    own_ref[...] = own
    ma = gram_of(own[:32])
    mab = ma + gram_of(own[32:])
    eye = jnp.where(
        lax.broadcasted_iota(jnp.int32, (128, 128), 0) == lax.broadcasted_iota(jnp.int32, (128, 128), 1), 1.0, 0.0
    )
    count = jnp.full((128, 128), 64 * w, jnp.int32).astype(jnp.float32)
    inv_a, inv_b = 1.0 / (count + 32.0), 1.0 / (count + 64.0)
    own_a, own_b = eye + ma * inv_a, eye + mab * inv_b
    for v in range(15):
        @pl.when(v < w)
        def _():
            rdma(gath.at[v], gath.at[v], xy_send.at[v], xy_recv.at[v], {"win": v}).wait_recv()
    gram_send[...] = gram_split(gath[...].reshape(512, 128))
    swap = rdma(gram_send, gram_recv, pair_sem.at[0], pair_sem.at[1], {"dof": partner})
    swap.start()
    rdma(part.at[fifteen], rs_buf.at[fifteen], rs_send, rs_recv, {"dof": partner}).wait_send()
    rdma(ag_buf.at[fifteen], ag_buf.at[fifteen], ag_send, ag_other, {"dof": partner}).wait_send()
    for v in range(1, 16):
        @pl.when(v > w)
        def _():
            rdma(ag_buf.at[eight], gath.at[w], xy_send.at[v], xy_recv.at[v], {"win": v}).wait_send()
    swap.wait()
    base = gram_send[...] + gram_recv[...]
    grams_ref[0] = own_a + base * inv_a
    grams_ref[1] = own_b + base * inv_b


def sum_call(snapshots, sketch_matrix):
    depth = sketch_matrix.shape[0] // CHUNKS
    f32 = jnp.float32
    return pl.pallas_call(
        sum_kernel,
        out_shape=(jax.ShapeDtypeStruct((64, 128), f32), jax.ShapeDtypeStruct((2, 128, 128), f32)),
        in_specs=[pl.BlockSpec(memory_space=pl.ANY)] * 2,
        out_specs=(pl.BlockSpec(memory_space=pltpu.VMEM),) * 2,
        scratch_shapes=[
            pltpu.VMEM((CHUNKS, 64, depth), jnp.bfloat16),
            pltpu.VMEM((CHUNKS, depth, 128), jnp.bfloat16),
            pltpu.VMEM((16, 4, 128), f32),
            pltpu.VMEM((16, 4, 128), f32),
            pltpu.VMEM((16, 4, 128), f32),
            pltpu.VMEM((16, 8, 4, 128), f32),
            pltpu.VMEM((128, 128), f32),
            pltpu.VMEM((128, 128), f32),
            pltpu.SemaphoreType.DMA((2, CHUNKS)),
            pltpu.SemaphoreType.DMA,
            pltpu.SemaphoreType.DMA,
            pltpu.SemaphoreType.DMA,
            pltpu.SemaphoreType.DMA((8,)),
            pltpu.SemaphoreType.DMA,
            pltpu.SemaphoreType.DMA((16,)),
            pltpu.SemaphoreType.DMA((16,)),
            pltpu.SemaphoreType.DMA((2,)),
        ],
        compiler_params=pltpu.CompilerParams(collective_id=0, has_side_effects=True, vmem_limit_bytes=52 * 1024 * 1024),
    )(snapshots.T, sketch_matrix)

def solve_kernel(own_ref, grams_ref, pivots_ref, sing_ref, proj_ref):
    piv = pivots_ref[...]
    piv_row = jnp.concatenate([piv[0:1, :], piv[1:2, :]], axis=1)
    sing, proj = solve_windows(grams_ref[0], grams_ref[1], own_ref[:32, :], own_ref[32:, :], piv_row)
    sing_ref[...] = sing
    proj_ref[0] = proj[:, :64]
    proj_ref[1] = proj[:, 64:]


def local(snapshots, sketch_matrix, pivots):
    own, grams = sum_call(snapshots, sketch_matrix)
    sing, proj = pl.pallas_call(
        solve_kernel,
        out_shape=(jax.ShapeDtypeStruct((2, 64), jnp.float32), jax.ShapeDtypeStruct((2, 32, 64), jnp.float32)),
        in_specs=[pl.BlockSpec(memory_space=pltpu.VMEM)] * 3,
        out_specs=(pl.BlockSpec(memory_space=pltpu.VMEM),) * 2,
        compiler_params=pltpu.CompilerParams(vmem_limit_bytes=16 * 1024 * 1024),
    )(own, grams, pivots)
    return sing, jnp.swapaxes(proj, 1, 2)


def solution(mesh):
    placed = (P("dof", "win"), P("dof", None), P("win", None))
    return jax.shard_map(
        local,
        mesh=mesh,
        in_specs=placed,
        out_specs=(P("win", None), P("win", None, None)),
        check_vma=False,
    )
```

```python
import functools
import math

import jax
import jax.numpy as jnp
from jax import lax
from jax.experimental import pallas as pl
from jax.experimental.pallas import tpu as pltpu
from jax.sharding import PartitionSpec as P

HIGHEST_PREC = lax.Precision.HIGHEST
RANK = 64
NT = (((1,), (1,)), ((), ()))


def dot_nt(a, b):
    return lax.dot_general(a, b, NT, precision=HIGHEST_PREC, preferred_element_type=jnp.float32)


def dot_nn(a, b):
    return lax.dot_general(a, b, (((1,), (0,)), ((), ())), precision=HIGHEST_PREC, preferred_element_type=jnp.float32)


def dot_bf16(a, b, dims=(((1,), (0,)), ((), ()))):
    return lax.dot_general(a, b, dims, preferred_element_type=jnp.float32)


def two_terms(x):
    high = x.astype(jnp.bfloat16)
    return high, (x - high.astype(jnp.float32)).astype(jnp.bfloat16)


def three_terms(x):
    high = x.astype(jnp.bfloat16)
    rest = x - high.astype(jnp.float32)
    mid = rest.astype(jnp.bfloat16)
    return high, mid, (rest - mid.astype(jnp.float32)).astype(jnp.bfloat16)


def dot_full(a, b, dims=(((1,), (0,)), ((), ()))):
    rows = a[0].shape[0]
    x = dot_bf16(jnp.concatenate(a, axis=0), b[0], dims)
    y = dot_bf16(jnp.concatenate(a[:2], axis=0), b[1], dims)
    z = dot_bf16(a[0], b[2], dims)
    return x[:rows] + ((x[rows : 2 * rows] + y[:rows]) + (x[2 * rows :] + y[rows:] + z))


def halves(a, b):
    return jnp.concatenate([a[:, :64], b[:, :64]], axis=1), jnp.concatenate([a[:, 64:], b[:, 64:]], axis=1)


def split_rows(x):
    return [x[8 * i : 8 * i + 8, :] for i in range(8)]


def whiten(gram, *payload):
    lane = lax.broadcasted_iota(jnp.int32, (8, 128), 1)
    sub = lax.broadcasted_iota(jnp.int32, (8, 128), 0)
    base = lane - lane % 64
    small = 2.0**-32
    if gram is None:
        rows = [split_rows(x * small) for x in payload]
        pivots_from, unit = rows[0], 2.0**16
    else:
        rows = [split_rows(x) for x in payload]
        pivots_from, unit = split_rows(gram * small), 2.0**-16

    def bcast(x, p):
        return jnp.broadcast_to(x[p : p + 1, :], (8, 128))

    for kb in range(8):
        cols = []
        for j in range(8):
            idx = base + (8 * kb + j)
            cols.append({i: jnp.take_along_axis(pivots_from[i], idx, axis=1) for i in range(kb, 8)})
        diag = None
        for p in range(0, 8, 2):
            q = p + 1
            cp, cq = cols[p], cols[q]
            a, b, c = bcast(cp[kb], p), bcast(cp[kb], q), bcast(cq[kb], q)
            det = a * c - b * b
            inv = 1.0 / det
            inv_a = 1.0 / a
            m1, m2 = {}, {}
            for i in range(kb, 8):
                n1 = cp[i] * c - cq[i] * b
                n2 = cq[i] * a - cp[i] * b
                if i == kb:
                    n1 = jnp.where(sub > q, n1, 0.0)
                    n2 = jnp.where(sub > q, n2, 0.0)
                m1[i], m2[i] = n1 * inv, n2 * inv
            m1[kb] = jnp.where(sub == q, b * inv_a, m1[kb])
            dq = det * inv_a
            diag = a if diag is None else jnp.where(sub >= p, a, diag)
            diag = jnp.where(sub >= q, dq, diag)
            for j in range(q + 1, 8):
                rp, rq = bcast(cols[j][kb], p), bcast(cols[j][kb], q)
                for i in range(kb, 8):
                    cols[j][i] = cols[j][i] - (m1[i] * rp + m2[i] * rq)
            for v in rows if gram is None or kb == 7 else [pivots_from] + rows:
                rp, rq = bcast(v[kb], p), bcast(v[kb], q)
                for i in range(kb, 8):
                    v[i] = v[i] - (m1[i] * rp + m2[i] * rq)
        scale = lax.rsqrt(diag) * unit
        for v in rows:
            v[kb] = v[kb] * scale
    return [jnp.concatenate(v, axis=0) for v in rows]


def masked_pair(low, high):
    first = lax.broadcasted_iota(jnp.int32, (64, 128), 1) < 64
    zero = jnp.zeros((64, 128), low.dtype)
    top = jnp.concatenate([jnp.where(first, low, zero), jnp.where(first, high, zero)], axis=1)
    bottom = jnp.concatenate([jnp.where(first, zero, low), jnp.where(first, zero, high)], axis=1)
    return jnp.concatenate([top, bottom], axis=0)


def solve_windows(pa, pb, za, zb, pivots_row):
    alo, ahi = halves(pa, pb)
    zero = jnp.zeros((64, 64), jnp.float32)

    def block_rows(x, first):
        left = jnp.concatenate([x[:, :64], zero] if first else [zero, x[:, 64:]], axis=1)
        return left

    lo_a, lo_b = alo[:64], alo[64:]
    hi_a, hi_b = ahi[:64], ahi[64:]
    joint = jnp.concatenate(
        [
            jnp.concatenate([block_rows(lo_a, True), block_rows(hi_a, True)], axis=1),
            jnp.concatenate([block_rows(lo_a, False), block_rows(hi_a, False)], axis=1),
            jnp.concatenate([block_rows(lo_b, True), block_rows(hi_b, True)], axis=1),
            jnp.concatenate([block_rows(lo_b, False), block_rows(hi_b, False)], axis=1),
        ],
        axis=0,
    )
    joint_terms = three_terms(joint)
    joint_hi, joint_lo = joint_terms[:2]
    first = lax.broadcasted_iota(jnp.int32, (8, 128), 1) < 64
    row = lax.broadcasted_iota(jnp.int32, (8, 128), 0)
    pick = (jnp.where((row == 0) & first, 1.0, 0.0) + jnp.where((row == 1) & (~first), 1.0, 0.0)).astype(jnp.bfloat16)
    j = lax.broadcasted_iota(jnp.int32, (256, 128), 0)
    lane = lax.broadcasted_iota(jnp.int32, (256, 128), 1)
    own = (j // 64) % 2 == lane // 64
    dim = j % 64 + 64 * (j // 128)
    onehot = jnp.where(own & (dim == pivots_row), 1.0, 0.0).astype(jnp.bfloat16)
    r = lax.broadcasted_iota(jnp.int32, (64, 128), 0)
    c = lax.broadcasted_iota(jnp.int32, (64, 128), 1)
    diagonal = c % 64 == r
    z_hi, z_lo = two_terms(jnp.concatenate(halves(za, zb), axis=1))
    square = dot_full(three_terms(jnp.concatenate([lo_a, hi_a], axis=1)), joint_terms)
    low, high = whiten(None, square[:, :128], square[:, 128:])
    image = three_terms(jnp.concatenate([low, high], axis=1))
    gram = dot_full(image, [masked_pair(t[:, :128], t[:, 128:]) for t in image], NT)
    low, high = whiten(gram, low, high)
    basis = jnp.concatenate([low, high], axis=1)
    basis_hi, basis_lo = two_terms(basis)
    both = jnp.concatenate([basis_hi, basis_lo], axis=0)
    image = dot_bf16(both, joint_hi)
    image = image[:64] + (image[64:] + dot_bf16(basis_hi, joint_lo))
    prod = low * image[:, :128] + high * image[:, 128:]
    prod_hi, prod_lo = two_terms(prod)
    squares = dot_bf16(pick, prod_hi, NT) + dot_bf16(pick, prod_lo, NT)
    picked = dot_bf16(both, onehot)
    picked = picked[:64] + picked[64:]
    weight = jnp.sum(jnp.where(diagonal, picked, 0.0), axis=0, keepdims=True) * math.sqrt(128)
    pair_hi, pair_lo = masked_pair(basis_hi[:, :128], basis_hi[:, 128:]), masked_pair(basis_lo[:, :128], basis_lo[:, 128:])
    proj = dot_bf16(jnp.concatenate([z_hi, z_lo], axis=0), pair_hi, NT)
    proj = (proj[:32] + (proj[32:] + dot_bf16(z_hi, pair_lo, NT))) * weight
    return jnp.sqrt(squares[:2]), proj


MESH = pl.DeviceIdType.MESH
CHUNKS = 8


def rdma(src, dst, send, recv, where):
    return pltpu.make_async_remote_copy(
        src_ref=src, dst_ref=dst, send_sem=send, recv_sem=recv, device_id=where, device_id_type=MESH
    )


def gram_of(x):
    return lax.dot_general(
        x, x, (((0,), (0,)), ((), ())), precision=lax.Precision.HIGHEST, preferred_element_type=jnp.float32
    )


def gram_split(x):
    high = x.astype(jnp.bfloat16)
    low = (x - high.astype(jnp.float32)).astype(jnp.bfloat16)
    both = jnp.concatenate([high, low], axis=1)
    g = lax.dot_general(both, both, (((0,), (0,)), ((), ())), preferred_element_type=jnp.float32)
    return (g[:128, :128] + g[128:, 128:]) + (g[:128, 128:] + g[128:, :128])


def slot_of(q):
    return lax.rem(q, 2) * 8 + q // 2


def sum_kernel(snap_hbm, sketch_hbm, own_ref, grams_ref,
               snap, sketch, part, rs_buf, ag_buf, gath, gram_send, gram_recv,
               in_sem, rs_send, rs_recv, ag_send, ag_recv, ag_other, xy_send, xy_recv, pair_sem):
    d = lax.axis_index("dof")
    w = lax.axis_index("win")
    nd, nw = 16, 16
    core = lax.rem(d, 2)
    partner = d + 1 - 2 * core
    depth = sketch.shape[1]
    loads = []
    for i in range(CHUNKS):
        a = pltpu.make_async_copy(sketch_hbm.at[pl.ds(i * depth, depth), :], sketch.at[i], in_sem.at[0, i])
        b = pltpu.make_async_copy(snap_hbm.at[:, pl.ds(i * depth, depth)], snap.at[i], in_sem.at[1, i])
        a.start()
        b.start()
        loads.append((a, b))
    gath[...] = jnp.zeros_like(gath)
    barrier = pltpu.get_barrier_semaphore()
    for k in range(1, 16):
        pl.semaphore_signal(barrier, inc=1, device_id={"dof": lax.rem(d + k, nd)}, device_id_type=MESH)
        pl.semaphore_signal(barrier, inc=1, device_id={"win": lax.rem(w + k, nw)}, device_id_type=MESH)
    total = jnp.zeros((64, 128), jnp.float32)
    for i in range(CHUNKS):
        for copy in loads[i]:
            copy.wait()
        total = total + jnp.dot(snap[i], sketch[i], preferred_element_type=jnp.float32)
    for p in range(16):
        part[p] = total[4 * p : 4 * p + 4, :]
    pl.semaphore_wait(barrier, 30)
    me = slot_of(d)
    order = [8, 9, 7, 6, 10, 5, 11, 4, 12, 3, 13, 2, 14, 15, 1]
    for k in order:
        q = lax.rem(d + k, nd)
        rdma(part.at[slot_of(q)], rs_buf.at[me], rs_send, rs_recv, {"dof": q}).start()
    rs_buf[me] = part[me]
    fifteen = pl.ds(0, 15)
    rdma(part.at[fifteen], rs_buf.at[fifteen], rs_send, rs_recv, {"dof": partner}).wait_recv()
    ag_buf[me] = jnp.sum(rs_buf[...], axis=0)
    z_here = d // 2
    for k in order:
        q = lax.rem(d + k, nd)
        arrival = ag_other if k % 2 else ag_recv.at[z_here]
        rdma(ag_buf.at[me], ag_buf.at[me], ag_send, arrival, {"dof": q}).start()

    def wait_piece(q):
        rdma(ag_buf.at[slot_of(q)], ag_buf.at[slot_of(q)], ag_send, ag_recv.at[q // 2], {"dof": q}).wait_recv()

    def forward(first, count):
        src = ag_buf.at[pl.ds(core * 8 + first, count)]
        dst = gath.at[w, pl.ds(first, count)]

        def send(v, carry):
            rdma(src, dst, xy_send.at[v], xy_recv.at[w], {"win": v}).start()
            return carry

        lax.fori_loop(w + 1, 16, send, 0)

    forward(z_here, 1)
    for k in reversed(order):
        if k % 2 == 0:
            q = lax.rem(d + k, nd)
            wait_piece(q)
            forward(q // 2, 1)
    eight = pl.ds(0, 8)
    rdma(ag_buf.at[eight], ag_buf.at[eight], ag_send, ag_other, {"dof": partner}).wait_recv()
    own = ag_buf[...].reshape(64, 128)
    own_ref[...] = own
    ma = gram_of(own[:32])
    mab = ma + gram_of(own[32:])
    eye = jnp.where(
        lax.broadcasted_iota(jnp.int32, (128, 128), 0) == lax.broadcasted_iota(jnp.int32, (128, 128), 1), 1.0, 0.0
    )
    count = jnp.full((128, 128), 64 * w, jnp.int32).astype(jnp.float32)
    inv_a, inv_b = 1.0 / (count + 32.0), 1.0 / (count + 64.0)
    own_a, own_b = eye + ma * inv_a, eye + mab * inv_b
    for v in range(15):
        @pl.when(v < w)
        def _():
            rdma(gath.at[v], gath.at[v], xy_send.at[v], xy_recv.at[v], {"win": v}).wait_recv()
    gram_send[...] = gram_split(gath[...].reshape(512, 128))
    swap = rdma(gram_send, gram_recv, pair_sem.at[0], pair_sem.at[1], {"dof": partner})
    swap.start()
    rdma(part.at[fifteen], rs_buf.at[fifteen], rs_send, rs_recv, {"dof": partner}).wait_send()
    rdma(ag_buf.at[fifteen], ag_buf.at[fifteen], ag_send, ag_other, {"dof": partner}).wait_send()
    for v in range(1, 16):
        @pl.when(v > w)
        def _():
            rdma(ag_buf.at[eight], gath.at[w], xy_send.at[v], xy_recv.at[v], {"win": v}).wait_send()
    swap.wait()
    base = gram_send[...] + gram_recv[...]
    grams_ref[0] = own_a + base * inv_a
    grams_ref[1] = own_b + base * inv_b


def sum_call(snapshots, sketch_matrix):
    depth = sketch_matrix.shape[0] // CHUNKS
    f32 = jnp.float32
    return pl.pallas_call(
        sum_kernel,
        out_shape=(jax.ShapeDtypeStruct((64, 128), f32), jax.ShapeDtypeStruct((2, 128, 128), f32)),
        in_specs=[pl.BlockSpec(memory_space=pl.ANY)] * 2,
        out_specs=(pl.BlockSpec(memory_space=pltpu.VMEM),) * 2,
        scratch_shapes=[
            pltpu.VMEM((CHUNKS, 64, depth), jnp.bfloat16),
            pltpu.VMEM((CHUNKS, depth, 128), jnp.bfloat16),
            pltpu.VMEM((16, 4, 128), f32),
            pltpu.VMEM((16, 4, 128), f32),
            pltpu.VMEM((16, 4, 128), f32),
            pltpu.VMEM((16, 8, 4, 128), f32),
            pltpu.VMEM((128, 128), f32),
            pltpu.VMEM((128, 128), f32),
            pltpu.SemaphoreType.DMA((2, CHUNKS)),
            pltpu.SemaphoreType.DMA,
            pltpu.SemaphoreType.DMA,
            pltpu.SemaphoreType.DMA,
            pltpu.SemaphoreType.DMA((8,)),
            pltpu.SemaphoreType.DMA,
            pltpu.SemaphoreType.DMA((16,)),
            pltpu.SemaphoreType.DMA((16,)),
            pltpu.SemaphoreType.DMA((2,)),
        ],
        compiler_params=pltpu.CompilerParams(collective_id=0, has_side_effects=True, vmem_limit_bytes=52 * 1024 * 1024),
    )(snapshots.T, sketch_matrix)

def solve_kernel(own_ref, grams_ref, pivots_ref, sing_ref, proj_ref):
    piv = pivots_ref[...]
    piv_row = jnp.concatenate([piv[0:1, :], piv[1:2, :]], axis=1)
    sing, proj = solve_windows(grams_ref[0], grams_ref[1], own_ref[:32, :], own_ref[32:, :], piv_row)
    sing_ref[...] = sing
    proj_ref[0] = proj[:, :64]
    proj_ref[1] = proj[:, 64:]


def local(snapshots, sketch_matrix, pivots):
    own, grams = sum_call(snapshots, sketch_matrix)
    sing, proj = pl.pallas_call(
        solve_kernel,
        out_shape=(jax.ShapeDtypeStruct((2, 64), jnp.float32), jax.ShapeDtypeStruct((2, 32, 64), jnp.float32)),
        in_specs=[pl.BlockSpec(memory_space=pltpu.VMEM)] * 3,
        out_specs=(pl.BlockSpec(memory_space=pltpu.VMEM),) * 2,
        compiler_params=pltpu.CompilerParams(vmem_limit_bytes=16 * 1024 * 1024),
    )(own, grams, pivots)
    return sing, jnp.swapaxes(proj, 1, 2)


def solution(mesh):
    placed = (P("dof", "win"), P("dof", None), P("win", None))
    return jax.shard_map(
        local,
        mesh=mesh,
        in_specs=placed,
        out_specs=(P("win", None), P("win", None, None)),
        check_vma=False,
    )
```

```python
import functools
import math

import jax
import jax.numpy as jnp
from jax import lax
from jax.experimental import pallas as pl
from jax.experimental.pallas import tpu as pltpu
from jax.sharding import PartitionSpec as P

HIGHEST_PREC = lax.Precision.HIGHEST
RANK = 64
NT = (((1,), (1,)), ((), ()))


def dot_nt(a, b):
    return lax.dot_general(a, b, NT, precision=HIGHEST_PREC, preferred_element_type=jnp.float32)


def dot_nn(a, b):
    return lax.dot_general(a, b, (((1,), (0,)), ((), ())), precision=HIGHEST_PREC, preferred_element_type=jnp.float32)


def dot_bf16(a, b, dims=(((1,), (0,)), ((), ()))):
    return lax.dot_general(a, b, dims, preferred_element_type=jnp.float32)


def two_terms(x):
    high = x.astype(jnp.bfloat16)
    return high, (x - high.astype(jnp.float32)).astype(jnp.bfloat16)


def three_terms(x):
    high = x.astype(jnp.bfloat16)
    rest = x - high.astype(jnp.float32)
    mid = rest.astype(jnp.bfloat16)
    return high, mid, (rest - mid.astype(jnp.float32)).astype(jnp.bfloat16)


def dot_full(a, b, dims=(((1,), (0,)), ((), ()))):
    rows = a[0].shape[0]
    x = dot_bf16(jnp.concatenate(a, axis=0), b[0], dims)
    y = dot_bf16(jnp.concatenate(a[:2], axis=0), b[1], dims)
    z = dot_bf16(a[0], b[2], dims)
    return x[:rows] + ((x[rows : 2 * rows] + y[:rows]) + (x[2 * rows :] + y[rows:] + z))


def halves(a, b):
    return jnp.concatenate([a[:, :64], b[:, :64]], axis=1), jnp.concatenate([a[:, 64:], b[:, 64:]], axis=1)


def split_rows(x):
    return [x[8 * i : 8 * i + 8, :] for i in range(8)]


def whiten(gram, *payload):
    lane = lax.broadcasted_iota(jnp.int32, (8, 128), 1)
    sub = lax.broadcasted_iota(jnp.int32, (8, 128), 0)
    base = lane - lane % 64
    small = 2.0**-32
    if gram is None:
        rows = [split_rows(x * small) for x in payload]
        pivots_from, unit = rows[0], 2.0**16
    else:
        rows = [split_rows(x) for x in payload]
        pivots_from, unit = split_rows(gram * small), 2.0**-16

    def bcast(x, p):
        return jnp.broadcast_to(x[p : p + 1, :], (8, 128))

    for kb in range(8):
        cols = []
        for j in range(8):
            idx = base + (8 * kb + j)
            cols.append({i: jnp.take_along_axis(pivots_from[i], idx, axis=1) for i in range(kb, 8)})
        diag = None
        for p in range(0, 8, 2):
            q = p + 1
            cp, cq = cols[p], cols[q]
            a, b, c = bcast(cp[kb], p), bcast(cp[kb], q), bcast(cq[kb], q)
            det = a * c - b * b
            inv = 1.0 / det
            inv_a = 1.0 / a
            m1, m2 = {}, {}
            for i in range(kb, 8):
                n1 = cp[i] * c - cq[i] * b
                n2 = cq[i] * a - cp[i] * b
                if i == kb:
                    n1 = jnp.where(sub > q, n1, 0.0)
                    n2 = jnp.where(sub > q, n2, 0.0)
                m1[i], m2[i] = n1 * inv, n2 * inv
            m1[kb] = jnp.where(sub == q, b * inv_a, m1[kb])
            dq = det * inv_a
            diag = a if diag is None else jnp.where(sub >= p, a, diag)
            diag = jnp.where(sub >= q, dq, diag)
            for j in range(q + 1, 8):
                rp, rq = bcast(cols[j][kb], p), bcast(cols[j][kb], q)
                for i in range(kb, 8):
                    cols[j][i] = cols[j][i] - (m1[i] * rp + m2[i] * rq)
            for v in rows if gram is None or kb == 7 else [pivots_from] + rows:
                rp, rq = bcast(v[kb], p), bcast(v[kb], q)
                for i in range(kb, 8):
                    v[i] = v[i] - (m1[i] * rp + m2[i] * rq)
        scale = lax.rsqrt(diag) * unit
        for v in rows:
            v[kb] = v[kb] * scale
    return [jnp.concatenate(v, axis=0) for v in rows]


def masked_pair(low, high):
    first = lax.broadcasted_iota(jnp.int32, (64, 128), 1) < 64
    zero = jnp.zeros((64, 128), low.dtype)
    top = jnp.concatenate([jnp.where(first, low, zero), jnp.where(first, high, zero)], axis=1)
    bottom = jnp.concatenate([jnp.where(first, zero, low), jnp.where(first, zero, high)], axis=1)
    return jnp.concatenate([top, bottom], axis=0)


def solve_windows(pa, pb, za, zb, pivots_row):
    alo, ahi = halves(pa, pb)
    zero = jnp.zeros((64, 64), jnp.float32)

    def block_rows(x, first):
        left = jnp.concatenate([x[:, :64], zero] if first else [zero, x[:, 64:]], axis=1)
        return left

    lo_a, lo_b = alo[:64], alo[64:]
    hi_a, hi_b = ahi[:64], ahi[64:]
    joint = jnp.concatenate(
        [
            jnp.concatenate([block_rows(lo_a, True), block_rows(hi_a, True)], axis=1),
            jnp.concatenate([block_rows(lo_a, False), block_rows(hi_a, False)], axis=1),
            jnp.concatenate([block_rows(lo_b, True), block_rows(hi_b, True)], axis=1),
            jnp.concatenate([block_rows(lo_b, False), block_rows(hi_b, False)], axis=1),
        ],
        axis=0,
    )
    joint_terms = three_terms(joint)
    joint_hi, joint_lo = joint_terms[:2]
    first = lax.broadcasted_iota(jnp.int32, (8, 128), 1) < 64
    row = lax.broadcasted_iota(jnp.int32, (8, 128), 0)
    pick = (jnp.where((row == 0) & first, 1.0, 0.0) + jnp.where((row == 1) & (~first), 1.0, 0.0)).astype(jnp.bfloat16)
    j = lax.broadcasted_iota(jnp.int32, (256, 128), 0)
    lane = lax.broadcasted_iota(jnp.int32, (256, 128), 1)
    own = (j // 64) % 2 == lane // 64
    dim = j % 64 + 64 * (j // 128)
    onehot = jnp.where(own & (dim == pivots_row), 1.0, 0.0).astype(jnp.bfloat16)
    r = lax.broadcasted_iota(jnp.int32, (64, 128), 0)
    c = lax.broadcasted_iota(jnp.int32, (64, 128), 1)
    diagonal = c % 64 == r
    z_hi, z_lo = two_terms(jnp.concatenate(halves(za, zb), axis=1))
    square = dot_full(three_terms(jnp.concatenate([lo_a, hi_a], axis=1)), joint_terms)
    low, high = whiten(None, square[:, :128], square[:, 128:])
    image = three_terms(jnp.concatenate([low, high], axis=1))
    gram = dot_full(image, [masked_pair(t[:, :128], t[:, 128:]) for t in image], NT)
    low, high = whiten(gram, low, high)
    basis = jnp.concatenate([low, high], axis=1)
    basis_hi, basis_lo = two_terms(basis)
    both = jnp.concatenate([basis_hi, basis_lo], axis=0)
    image = dot_bf16(both, joint_hi)
    image = image[:64] + (image[64:] + dot_bf16(basis_hi, joint_lo))
    prod = low * image[:, :128] + high * image[:, 128:]
    prod_hi, prod_lo = two_terms(prod)
    squares = dot_bf16(pick, prod_hi, NT) + dot_bf16(pick, prod_lo, NT)
    picked = dot_bf16(both, onehot)
    picked = picked[:64] + picked[64:]
    weight = jnp.sum(jnp.where(diagonal, picked, 0.0), axis=0, keepdims=True) * math.sqrt(128)
    pair_hi, pair_lo = masked_pair(basis_hi[:, :128], basis_hi[:, 128:]), masked_pair(basis_lo[:, :128], basis_lo[:, 128:])
    proj = dot_bf16(jnp.concatenate([z_hi, z_lo], axis=0), pair_hi, NT)
    proj = (proj[:32] + (proj[32:] + dot_bf16(z_hi, pair_lo, NT))) * weight
    return jnp.sqrt(squares[:2]), proj


MESH = pl.DeviceIdType.MESH
CHUNKS = 8


def rdma(src, dst, send, recv, where):
    return pltpu.make_async_remote_copy(
        src_ref=src, dst_ref=dst, send_sem=send, recv_sem=recv, device_id=where, device_id_type=MESH
    )


def gram_of(x):
    return lax.dot_general(
        x, x, (((0,), (0,)), ((), ())), precision=lax.Precision.HIGHEST, preferred_element_type=jnp.float32
    )


def gram_split(x):
    high = x.astype(jnp.bfloat16)
    low = (x - high.astype(jnp.float32)).astype(jnp.bfloat16)
    both = jnp.concatenate([high, low], axis=1)
    g = lax.dot_general(both, both, (((0,), (0,)), ((), ())), preferred_element_type=jnp.float32)
    return (g[:128, :128] + g[128:, 128:]) + (g[:128, 128:] + g[128:, :128])


def slot_of(q):
    return lax.rem(q, 2) * 8 + q // 2


def sum_kernel(snap_hbm, sketch_hbm, own_ref, grams_ref,
               snap, sketch, part, rs_buf, ag_buf, gath, gram_send, gram_recv,
               in_sem, rs_send, rs_recv, ag_send, ag_recv, ag_other, xy_send, xy_recv, pair_sem):
    d = lax.axis_index("dof")
    w = lax.axis_index("win")
    nd, nw = 16, 16
    core = lax.rem(d, 2)
    partner = d + 1 - 2 * core
    depth = sketch.shape[0] // CHUNKS
    for i in range(CHUNKS):
        rows = pl.ds(i * depth, depth)
        pltpu.make_async_copy(sketch_hbm.at[rows, :], sketch.at[rows, :], in_sem.at[i]).start()
        pltpu.make_async_copy(snap_hbm.at[:, rows], snap.at[:, rows], in_sem.at[i]).start()
    gath[...] = jnp.zeros_like(gath)
    barrier = pltpu.get_barrier_semaphore()
    for k in range(1, 16):
        pl.semaphore_signal(barrier, inc=1, device_id={"dof": lax.rem(d + k, nd)}, device_id_type=MESH)
        pl.semaphore_signal(barrier, inc=1, device_id={"win": lax.rem(w + k, nw)}, device_id_type=MESH)
    total = jnp.zeros((64, 128), jnp.float32)
    chunk_bytes = pl.ds(0, depth + depth // 2)
    for i in range(CHUNKS):
        rows = pl.ds(i * depth, depth)
        pltpu.make_async_copy(sketch_hbm.at[chunk_bytes, :], sketch.at[chunk_bytes, :], in_sem.at[i]).wait()
        total = total + jnp.dot(snap[:, rows], sketch[rows, :], preferred_element_type=jnp.float32)
    for p in range(16):
        part[p] = total[4 * p : 4 * p + 4, :]
    pl.semaphore_wait(barrier, 30)
    me = slot_of(d)
    order = [8, 9, 7, 6, 10, 5, 11, 4, 12, 3, 13, 2, 14, 15, 1]
    for k in order:
        q = lax.rem(d + k, nd)
        rdma(part.at[slot_of(q)], rs_buf.at[me], rs_send, rs_recv, {"dof": q}).start()
    rs_buf[me] = part[me]
    fifteen = pl.ds(0, 15)
    rdma(part.at[fifteen], rs_buf.at[fifteen], rs_send, rs_recv, {"dof": partner}).wait_recv()
    ag_buf[me] = jnp.sum(rs_buf[...], axis=0)
    z_here = d // 2
    for k in order:
        q = lax.rem(d + k, nd)
        arrival = ag_other if k % 2 else ag_recv.at[z_here]
        rdma(ag_buf.at[me], ag_buf.at[me], ag_send, arrival, {"dof": q}).start()

    def wait_piece(q):
        rdma(ag_buf.at[slot_of(q)], ag_buf.at[slot_of(q)], ag_send, ag_recv.at[q // 2], {"dof": q}).wait_recv()

    def forward(first, count):
        src = ag_buf.at[pl.ds(core * 8 + first, count)]
        dst = gath.at[w, pl.ds(first, count)]

        def send(v, carry):
            rdma(src, dst, xy_send, xy_recv, {"win": v}).start()
            return carry

        lax.fori_loop(w + 1, 16, send, 0)

    forward(z_here, 1)
    for k in reversed(order):
        if k % 2 == 0:
            q = lax.rem(d + k, nd)
            wait_piece(q)
            forward(q // 2, 1)
    eight = pl.ds(0, 8)
    rdma(ag_buf.at[eight], ag_buf.at[eight], ag_send, ag_other, {"dof": partner}).wait_recv()
    own = ag_buf[...].reshape(64, 128)
    own_ref[...] = own
    ma = gram_of(own[:32])
    mab = ma + gram_of(own[32:])
    eye = jnp.where(
        lax.broadcasted_iota(jnp.int32, (128, 128), 0) == lax.broadcasted_iota(jnp.int32, (128, 128), 1), 1.0, 0.0
    )
    count = jnp.full((128, 128), 64 * w, jnp.int32).astype(jnp.float32)
    inv_a, inv_b = 1.0 / (count + 32.0), 1.0 / (count + 64.0)
    own_a, own_b = eye + ma * inv_a, eye + mab * inv_b

    def blocks(count):
        some = gath.at[pl.ds(0, count)]
        return rdma(some, some, xy_send, xy_recv, {"dof": partner})

    for count in range(1, 16):
        @pl.when(w == count)
        def _():
            blocks(count).wait_recv()
    gram_send[...] = gram_split(gath[...].reshape(512, 128))
    swap = rdma(gram_send, gram_recv, pair_sem.at[0], pair_sem.at[1], {"dof": partner})
    swap.start()
    rdma(part.at[fifteen], rs_buf.at[fifteen], rs_send, rs_recv, {"dof": partner}).wait_send()
    rdma(ag_buf.at[fifteen], ag_buf.at[fifteen], ag_send, ag_other, {"dof": partner}).wait_send()
    for count in range(1, 16):
        @pl.when(w == 15 - count)
        def _():
            blocks(count).wait_send()
    swap.wait()
    base = gram_send[...] + gram_recv[...]
    grams_ref[0] = own_a + base * inv_a
    grams_ref[1] = own_b + base * inv_b


def sum_call(snapshots, sketch_matrix):
    depth = sketch_matrix.shape[0] // CHUNKS
    f32 = jnp.float32
    return pl.pallas_call(
        sum_kernel,
        out_shape=(jax.ShapeDtypeStruct((64, 128), f32), jax.ShapeDtypeStruct((2, 128, 128), f32)),
        in_specs=[pl.BlockSpec(memory_space=pl.ANY)] * 2,
        out_specs=(pl.BlockSpec(memory_space=pltpu.VMEM),) * 2,
        scratch_shapes=[
            pltpu.VMEM((64, CHUNKS * depth), jnp.bfloat16),
            pltpu.VMEM((CHUNKS * depth, 128), jnp.bfloat16),
            pltpu.VMEM((16, 4, 128), f32),
            pltpu.VMEM((16, 4, 128), f32),
            pltpu.VMEM((16, 4, 128), f32),
            pltpu.VMEM((16, 8, 4, 128), f32),
            pltpu.VMEM((128, 128), f32),
            pltpu.VMEM((128, 128), f32),
            pltpu.SemaphoreType.DMA((CHUNKS,)),
            pltpu.SemaphoreType.DMA,
            pltpu.SemaphoreType.DMA,
            pltpu.SemaphoreType.DMA,
            pltpu.SemaphoreType.DMA((8,)),
            pltpu.SemaphoreType.DMA,
            pltpu.SemaphoreType.DMA,
            pltpu.SemaphoreType.DMA,
            pltpu.SemaphoreType.DMA((2,)),
        ],
        compiler_params=pltpu.CompilerParams(collective_id=0, has_side_effects=True, vmem_limit_bytes=52 * 1024 * 1024),
    )(snapshots.T, sketch_matrix)

def solve_kernel(own_ref, grams_ref, pivots_ref, sing_ref, proj_ref):
    piv = pivots_ref[...]
    piv_row = jnp.concatenate([piv[0:1, :], piv[1:2, :]], axis=1)
    sing, proj = solve_windows(grams_ref[0], grams_ref[1], own_ref[:32, :], own_ref[32:, :], piv_row)
    sing_ref[...] = sing
    proj_ref[0] = proj[:, :64]
    proj_ref[1] = proj[:, 64:]


def local(snapshots, sketch_matrix, pivots):
    own, grams = sum_call(snapshots, sketch_matrix)
    sing, proj = pl.pallas_call(
        solve_kernel,
        out_shape=(jax.ShapeDtypeStruct((2, 64), jnp.float32), jax.ShapeDtypeStruct((2, 32, 64), jnp.float32)),
        in_specs=[pl.BlockSpec(memory_space=pltpu.VMEM)] * 3,
        out_specs=(pl.BlockSpec(memory_space=pltpu.VMEM),) * 2,
        compiler_params=pltpu.CompilerParams(vmem_limit_bytes=16 * 1024 * 1024),
    )(own, grams, pivots)
    return sing, jnp.swapaxes(proj, 1, 2)


def solution(mesh):
    placed = (P("dof", "win"), P("dof", None), P("win", None))
    return jax.shard_map(
        local,
        mesh=mesh,
        in_specs=placed,
        out_specs=(P("win", None), P("win", None, None)),
        check_vma=False,
    )
```

```python
import functools
import math

import jax
import jax.numpy as jnp
from jax import lax
from jax.experimental import pallas as pl
from jax.experimental.pallas import tpu as pltpu
from jax.sharding import PartitionSpec as P

HIGHEST_PREC = lax.Precision.HIGHEST
RANK = 64
NT = (((1,), (1,)), ((), ()))


def dot_nt(a, b):
    return lax.dot_general(a, b, NT, precision=HIGHEST_PREC, preferred_element_type=jnp.float32)


def dot_nn(a, b):
    return lax.dot_general(a, b, (((1,), (0,)), ((), ())), precision=HIGHEST_PREC, preferred_element_type=jnp.float32)


def dot_bf16(a, b, dims=(((1,), (0,)), ((), ()))):
    return lax.dot_general(a, b, dims, preferred_element_type=jnp.float32)


def two_terms(x):
    high = x.astype(jnp.bfloat16)
    return high, (x - high.astype(jnp.float32)).astype(jnp.bfloat16)


def three_terms(x):
    high = x.astype(jnp.bfloat16)
    rest = x - high.astype(jnp.float32)
    mid = rest.astype(jnp.bfloat16)
    return high, mid, (rest - mid.astype(jnp.float32)).astype(jnp.bfloat16)


def dot_full(a, b, dims=(((1,), (0,)), ((), ()))):
    rows = a[0].shape[0]
    x = dot_bf16(jnp.concatenate(a, axis=0), b[0], dims)
    y = dot_bf16(jnp.concatenate(a[:2], axis=0), b[1], dims)
    z = dot_bf16(a[0], b[2], dims)
    return x[:rows] + ((x[rows : 2 * rows] + y[:rows]) + (x[2 * rows :] + y[rows:] + z))


def halves(a, b):
    return jnp.concatenate([a[:, :64], b[:, :64]], axis=1), jnp.concatenate([a[:, 64:], b[:, 64:]], axis=1)


def split_rows(x):
    return [x[8 * i : 8 * i + 8, :] for i in range(8)]


def whiten(gram, *payload):
    lane = lax.broadcasted_iota(jnp.int32, (8, 128), 1)
    sub = lax.broadcasted_iota(jnp.int32, (8, 128), 0)
    base = lane - lane % 64
    small = 2.0**-32
    if gram is None:
        rows = [split_rows(x * small) for x in payload]
        pivots_from, unit = rows[0], 2.0**16
    else:
        rows = [split_rows(x) for x in payload]
        pivots_from, unit = split_rows(gram * small), 2.0**-16

    def bcast(x, p):
        return jnp.broadcast_to(x[p : p + 1, :], (8, 128))

    for kb in range(8):
        cols = []
        for j in range(8):
            idx = base + (8 * kb + j)
            cols.append({i: jnp.take_along_axis(pivots_from[i], idx, axis=1) for i in range(kb, 8)})
        diag = None
        for p in range(0, 8, 2):
            q = p + 1
            cp, cq = cols[p], cols[q]
            a, b, c = bcast(cp[kb], p), bcast(cp[kb], q), bcast(cq[kb], q)
            det = a * c - b * b
            inv = 1.0 / det
            inv_a = 1.0 / a
            m1, m2 = {}, {}
            for i in range(kb, 8):
                n1 = cp[i] * c - cq[i] * b
                n2 = cq[i] * a - cp[i] * b
                if i == kb:
                    n1 = jnp.where(sub > q, n1, 0.0)
                    n2 = jnp.where(sub > q, n2, 0.0)
                m1[i], m2[i] = n1 * inv, n2 * inv
            m1[kb] = jnp.where(sub == q, b * inv_a, m1[kb])
            dq = det * inv_a
            diag = a if diag is None else jnp.where(sub >= p, a, diag)
            diag = jnp.where(sub >= q, dq, diag)
            for j in range(q + 1, 8):
                rp, rq = bcast(cols[j][kb], p), bcast(cols[j][kb], q)
                for i in range(kb, 8):
                    cols[j][i] = cols[j][i] - (m1[i] * rp + m2[i] * rq)
            for v in rows if gram is None or kb == 7 else [pivots_from] + rows:
                rp, rq = bcast(v[kb], p), bcast(v[kb], q)
                for i in range(kb, 8):
                    v[i] = v[i] - (m1[i] * rp + m2[i] * rq)
        scale = lax.rsqrt(diag) * unit
        for v in rows:
            v[kb] = v[kb] * scale
    return [jnp.concatenate(v, axis=0) for v in rows]


def masked_pair(low, high):
    first = lax.broadcasted_iota(jnp.int32, (64, 128), 1) < 64
    zero = jnp.zeros((64, 128), low.dtype)
    top = jnp.concatenate([jnp.where(first, low, zero), jnp.where(first, high, zero)], axis=1)
    bottom = jnp.concatenate([jnp.where(first, zero, low), jnp.where(first, zero, high)], axis=1)
    return jnp.concatenate([top, bottom], axis=0)


def solve_windows(pa, pb, za, zb, pivots_row):
    alo, ahi = halves(pa, pb)
    wide = jnp.concatenate([alo, ahi], axis=1)
    of_a = lax.broadcasted_iota(jnp.int32, (64, 256), 1) % 128 < 64

    def spread_rows(x):
        zero = jnp.zeros((64, 256), x.dtype)
        return jnp.concatenate(
            [jnp.where(of_a, x[:64], zero), jnp.where(of_a, zero, x[:64]), jnp.where(of_a, x[64:], zero), jnp.where(of_a, zero, x[64:])],
            axis=0,
        )

    wide_terms = three_terms(wide)
    joint_terms = [spread_rows(t) for t in wide_terms]
    joint_hi, joint_lo = joint_terms[:2]
    first = lax.broadcasted_iota(jnp.int32, (8, 128), 1) < 64
    row = lax.broadcasted_iota(jnp.int32, (8, 128), 0)
    pick = (jnp.where((row == 0) & first, 1.0, 0.0) + jnp.where((row == 1) & (~first), 1.0, 0.0)).astype(jnp.bfloat16)
    j = lax.broadcasted_iota(jnp.int32, (256, 128), 0)
    lane = lax.broadcasted_iota(jnp.int32, (256, 128), 1)
    own = (j // 64) % 2 == lane // 64
    dim = j % 64 + 64 * (j // 128)
    onehot = jnp.where(own & (dim == pivots_row), 1.0, 0.0).astype(jnp.bfloat16)
    r = lax.broadcasted_iota(jnp.int32, (64, 128), 0)
    c = lax.broadcasted_iota(jnp.int32, (64, 128), 1)
    diagonal = c % 64 == r
    z_hi, z_lo = two_terms(jnp.concatenate(halves(za, zb), axis=1))
    square = dot_full([t[:64] for t in wide_terms], joint_terms)
    low, high = whiten(None, square[:, :128], square[:, 128:])
    image = three_terms(jnp.concatenate([low, high], axis=1))
    gram = dot_full(image, [masked_pair(t[:, :128], t[:, 128:]) for t in image], NT)
    low, high = whiten(gram, low, high)
    basis = jnp.concatenate([low, high], axis=1)
    basis_hi, basis_lo = two_terms(basis)
    both = jnp.concatenate([basis_hi, basis_lo], axis=0)
    image = dot_bf16(both, joint_hi)
    image = image[:64] + (image[64:] + dot_bf16(basis_hi, joint_lo))
    prod = low * image[:, :128] + high * image[:, 128:]
    prod_hi, prod_lo = two_terms(prod)
    squares = dot_bf16(pick, prod_hi, NT) + dot_bf16(pick, prod_lo, NT)
    picked = dot_bf16(both, onehot)
    picked = picked[:64] + picked[64:]
    weight = jnp.sum(jnp.where(diagonal, picked, 0.0), axis=0, keepdims=True) * math.sqrt(128)
    pair_hi, pair_lo = masked_pair(basis_hi[:, :128], basis_hi[:, 128:]), masked_pair(basis_lo[:, :128], basis_lo[:, 128:])
    proj = dot_bf16(jnp.concatenate([z_hi, z_lo], axis=0), pair_hi, NT)
    proj = (proj[:32] + (proj[32:] + dot_bf16(z_hi, pair_lo, NT))) * weight
    return jnp.sqrt(squares[:2]), proj


MESH = pl.DeviceIdType.MESH
CHUNKS = 8


def rdma(src, dst, send, recv, where):
    return pltpu.make_async_remote_copy(
        src_ref=src, dst_ref=dst, send_sem=send, recv_sem=recv, device_id=where, device_id_type=MESH
    )


def gram_of(x):
    return lax.dot_general(
        x, x, (((0,), (0,)), ((), ())), precision=lax.Precision.HIGHEST, preferred_element_type=jnp.float32
    )


def gram_split(x):
    high = x.astype(jnp.bfloat16)
    low = (x - high.astype(jnp.float32)).astype(jnp.bfloat16)
    both = jnp.concatenate([high, low], axis=1)
    g = lax.dot_general(both, both, (((0,), (0,)), ((), ())), preferred_element_type=jnp.float32)
    return (g[:128, :128] + g[128:, 128:]) + (g[:128, 128:] + g[128:, :128])


def slot_of(q):
    return lax.rem(q, 2) * 8 + q // 2


def sum_kernel(snap_hbm, sketch_hbm, own_ref, grams_ref,
               snap, sketch, part, rs_buf, ag_buf, gath, gram_send, gram_recv,
               in_sem, rs_send, rs_recv, ag_send, ag_recv, ag_other, xy_send, xy_recv, pair_sem):
    d = lax.axis_index("dof")
    w = lax.axis_index("win")
    nd, nw = 16, 16
    core = lax.rem(d, 2)
    partner = d + 1 - 2 * core
    depth = sketch.shape[0] // CHUNKS
    for i in range(CHUNKS):
        rows = pl.ds(i * depth, depth)
        pltpu.make_async_copy(sketch_hbm.at[rows, :], sketch.at[rows, :], in_sem.at[i]).start()
        pltpu.make_async_copy(snap_hbm.at[:, rows], snap.at[:, rows], in_sem.at[i]).start()
    gath[...] = jnp.zeros_like(gath)
    barrier = pltpu.get_barrier_semaphore()
    for k in range(1, 16):
        pl.semaphore_signal(barrier, inc=1, device_id={"dof": lax.rem(d + k, nd)}, device_id_type=MESH)
        pl.semaphore_signal(barrier, inc=1, device_id={"win": lax.rem(w + k, nw)}, device_id_type=MESH)
    total = jnp.zeros((64, 128), jnp.float32)
    chunk_bytes = pl.ds(0, depth + depth // 2)
    for i in range(CHUNKS):
        rows = pl.ds(i * depth, depth)
        pltpu.make_async_copy(sketch_hbm.at[chunk_bytes, :], sketch.at[chunk_bytes, :], in_sem.at[i]).wait()
        total = total + jnp.dot(snap[:, rows], sketch[rows, :], preferred_element_type=jnp.float32)
    for p in range(16):
        part[p] = total[4 * p : 4 * p + 4, :]
    pl.semaphore_wait(barrier, 30)
    me = slot_of(d)
    order = [8, 9, 7, 6, 10, 5, 11, 4, 12, 3, 13, 2, 14, 15, 1]
    for k in order:
        q = lax.rem(d + k, nd)
        rdma(part.at[slot_of(q)], rs_buf.at[me], rs_send, rs_recv, {"dof": q}).start()
    rs_buf[me] = part[me]
    fifteen = pl.ds(0, 15)
    rdma(part.at[fifteen], rs_buf.at[fifteen], rs_send, rs_recv, {"dof": partner}).wait_recv()
    ag_buf[me] = jnp.sum(rs_buf[...], axis=0)
    z_here = d // 2
    for k in order:
        q = lax.rem(d + k, nd)
        arrival = ag_other if k % 2 else ag_recv.at[z_here]
        rdma(ag_buf.at[me], ag_buf.at[me], ag_send, arrival, {"dof": q}).start()

    def wait_piece(q):
        rdma(ag_buf.at[slot_of(q)], ag_buf.at[slot_of(q)], ag_send, ag_recv.at[q // 2], {"dof": q}).wait_recv()

    def forward(first, count):
        src = ag_buf.at[pl.ds(core * 8 + first, count)]
        dst = gath.at[w, pl.ds(first, count)]

        def send(v, carry):
            rdma(src, dst, xy_send, xy_recv, {"win": v}).start()
            return carry

        lax.fori_loop(w + 1, 16, send, 0)

    forward(z_here, 1)
    for k in reversed(order):
        if k % 2 == 0:
            q = lax.rem(d + k, nd)
            wait_piece(q)
            forward(q // 2, 1)
    eight = pl.ds(0, 8)
    rdma(ag_buf.at[eight], ag_buf.at[eight], ag_send, ag_other, {"dof": partner}).wait_recv()
    own = ag_buf[...].reshape(64, 128)
    own_ref[...] = own
    ma = gram_of(own[:32])
    mab = ma + gram_of(own[32:])
    eye = jnp.where(
        lax.broadcasted_iota(jnp.int32, (128, 128), 0) == lax.broadcasted_iota(jnp.int32, (128, 128), 1), 1.0, 0.0
    )
    count = jnp.full((128, 128), 64 * w, jnp.int32).astype(jnp.float32)
    inv_a, inv_b = 1.0 / (count + 32.0), 1.0 / (count + 64.0)
    own_a, own_b = eye + ma * inv_a, eye + mab * inv_b

    def blocks(count):
        some = gath.at[pl.ds(0, count)]
        return rdma(some, some, xy_send, xy_recv, {"dof": partner})

    for count in range(1, 16):
        @pl.when(w == count)
        def _():
            blocks(count).wait_recv()
    gram_send[...] = gram_split(gath[...].reshape(512, 128))
    swap = rdma(gram_send, gram_recv, pair_sem.at[0], pair_sem.at[1], {"dof": partner})
    swap.start()
    rdma(part.at[fifteen], rs_buf.at[fifteen], rs_send, rs_recv, {"dof": partner}).wait_send()
    rdma(ag_buf.at[fifteen], ag_buf.at[fifteen], ag_send, ag_other, {"dof": partner}).wait_send()
    for count in range(1, 16):
        @pl.when(w == 15 - count)
        def _():
            blocks(count).wait_send()
    swap.wait()
    base = gram_send[...] + gram_recv[...]
    grams_ref[0] = own_a + base * inv_a
    grams_ref[1] = own_b + base * inv_b


def sum_call(snapshots, sketch_matrix):
    depth = sketch_matrix.shape[0] // CHUNKS
    f32 = jnp.float32
    return pl.pallas_call(
        sum_kernel,
        out_shape=(jax.ShapeDtypeStruct((64, 128), f32), jax.ShapeDtypeStruct((2, 128, 128), f32)),
        in_specs=[pl.BlockSpec(memory_space=pl.ANY)] * 2,
        out_specs=(pl.BlockSpec(memory_space=pltpu.VMEM),) * 2,
        scratch_shapes=[
            pltpu.VMEM((64, CHUNKS * depth), jnp.bfloat16),
            pltpu.VMEM((CHUNKS * depth, 128), jnp.bfloat16),
            pltpu.VMEM((16, 4, 128), f32),
            pltpu.VMEM((16, 4, 128), f32),
            pltpu.VMEM((16, 4, 128), f32),
            pltpu.VMEM((16, 8, 4, 128), f32),
            pltpu.VMEM((128, 128), f32),
            pltpu.VMEM((128, 128), f32),
            pltpu.SemaphoreType.DMA((CHUNKS,)),
            pltpu.SemaphoreType.DMA,
            pltpu.SemaphoreType.DMA,
            pltpu.SemaphoreType.DMA,
            pltpu.SemaphoreType.DMA((8,)),
            pltpu.SemaphoreType.DMA,
            pltpu.SemaphoreType.DMA,
            pltpu.SemaphoreType.DMA,
            pltpu.SemaphoreType.DMA((2,)),
        ],
        compiler_params=pltpu.CompilerParams(collective_id=0, has_side_effects=True, vmem_limit_bytes=52 * 1024 * 1024),
    )(snapshots.T, sketch_matrix)

def solve_kernel(own_ref, grams_ref, pivots_ref, sing_ref, proj_ref):
    piv = pivots_ref[...]
    piv_row = jnp.concatenate([piv[0:1, :], piv[1:2, :]], axis=1)
    sing, proj = solve_windows(grams_ref[0], grams_ref[1], own_ref[:32, :], own_ref[32:, :], piv_row)
    sing_ref[...] = sing
    proj_ref[0] = proj[:, :64]
    proj_ref[1] = proj[:, 64:]


def local(snapshots, sketch_matrix, pivots):
    own, grams = sum_call(snapshots, sketch_matrix)
    sing, proj = pl.pallas_call(
        solve_kernel,
        out_shape=(jax.ShapeDtypeStruct((2, 64), jnp.float32), jax.ShapeDtypeStruct((2, 32, 64), jnp.float32)),
        in_specs=[pl.BlockSpec(memory_space=pltpu.VMEM)] * 3,
        out_specs=(pl.BlockSpec(memory_space=pltpu.VMEM),) * 2,
        compiler_params=pltpu.CompilerParams(vmem_limit_bytes=16 * 1024 * 1024),
    )(own, grams, pivots)
    return sing, jnp.swapaxes(proj, 1, 2)


def solution(mesh):
    placed = (P("dof", "win"), P("dof", None), P("win", None))
    return jax.shard_map(
        local,
        mesh=mesh,
        in_specs=placed,
        out_specs=(P("win", None), P("win", None, None)),
        check_vma=False,
    )
```

```python
import functools
import math

import jax
import jax.numpy as jnp
from jax import lax
from jax.experimental import pallas as pl
from jax.experimental.pallas import tpu as pltpu
from jax.sharding import PartitionSpec as P

HIGHEST_PREC = lax.Precision.HIGHEST
RANK = 64
NT = (((1,), (1,)), ((), ()))


def dot_nt(a, b):
    return lax.dot_general(a, b, NT, precision=HIGHEST_PREC, preferred_element_type=jnp.float32)


def dot_nn(a, b):
    return lax.dot_general(a, b, (((1,), (0,)), ((), ())), precision=HIGHEST_PREC, preferred_element_type=jnp.float32)


def dot_bf16(a, b, dims=(((1,), (0,)), ((), ()))):
    return lax.dot_general(a, b, dims, preferred_element_type=jnp.float32)


def two_terms(x):
    high = x.astype(jnp.bfloat16)
    return high, (x - high.astype(jnp.float32)).astype(jnp.bfloat16)


def three_terms(x):
    high = x.astype(jnp.bfloat16)
    rest = x - high.astype(jnp.float32)
    mid = rest.astype(jnp.bfloat16)
    return high, mid, (rest - mid.astype(jnp.float32)).astype(jnp.bfloat16)


def dot_full(a, b, dims=(((1,), (0,)), ((), ()))):
    rows = a[0].shape[0]
    x = dot_bf16(jnp.concatenate(a, axis=0), b[0], dims)
    y = dot_bf16(jnp.concatenate(a[:2], axis=0), b[1], dims)
    z = dot_bf16(a[0], b[2], dims)
    return x[:rows] + ((x[rows : 2 * rows] + y[:rows]) + (x[2 * rows :] + y[rows:] + z))


def halves(a, b):
    return jnp.concatenate([a[:, :64], b[:, :64]], axis=1), jnp.concatenate([a[:, 64:], b[:, 64:]], axis=1)


def split_rows(x):
    return [x[8 * i : 8 * i + 8, :] for i in range(8)]


def whiten(gram, *payload):
    lane = lax.broadcasted_iota(jnp.int32, (8, 128), 1)
    sub = lax.broadcasted_iota(jnp.int32, (8, 128), 0)
    base = lane - lane % 64
    small = 2.0**-32
    if gram is None:
        rows = [split_rows(x * small) for x in payload]
        pivots_from, unit = rows[0], 2.0**16
    else:
        rows = [split_rows(x) for x in payload]
        pivots_from, unit = split_rows(gram * small), 2.0**-16

    def bcast(x, p):
        return jnp.broadcast_to(x[p : p + 1, :], (8, 128))

    for kb in range(8):
        cols = [{} for _ in range(8)]
        for i in range(kb, 8):
            for j in range(8):
                cols[j][i] = jnp.take_along_axis(pivots_from[i], base + (8 * kb + j), axis=1)
        diag = None
        for p in range(0, 8, 2):
            q = p + 1
            cp, cq = cols[p], cols[q]
            a, b, c = bcast(cp[kb], p), bcast(cp[kb], q), bcast(cq[kb], q)
            det = a * c - b * b
            inv = 1.0 / det
            inv_a = 1.0 / a
            m1, m2 = {}, {}
            for i in range(kb, 8):
                n1 = cp[i] * c - cq[i] * b
                n2 = cq[i] * a - cp[i] * b
                if i == kb:
                    n1 = jnp.where(sub > q, n1, 0.0)
                    n2 = jnp.where(sub > q, n2, 0.0)
                m1[i], m2[i] = n1 * inv, n2 * inv
            m1[kb] = jnp.where(sub == q, b * inv_a, m1[kb])
            dq = det * inv_a
            diag = a if diag is None else jnp.where(sub >= p, a, diag)
            diag = jnp.where(sub >= q, dq, diag)
            for j in range(q + 1, 8):
                rp, rq = bcast(cols[j][kb], p), bcast(cols[j][kb], q)
                for i in range(kb, 8):
                    cols[j][i] = cols[j][i] - (m1[i] * rp + m2[i] * rq)
            for v in rows if gram is None or kb == 7 else [pivots_from] + rows:
                rp, rq = bcast(v[kb], p), bcast(v[kb], q)
                for i in range(kb, 8):
                    v[i] = v[i] - (m1[i] * rp + m2[i] * rq)
        scale = lax.rsqrt(diag) * unit
        for v in rows:
            v[kb] = v[kb] * scale
    return [jnp.concatenate(v, axis=0) for v in rows]


def masked_pair(low, high):
    first = lax.broadcasted_iota(jnp.int32, (64, 128), 1) < 64
    zero = jnp.zeros((64, 128), low.dtype)
    top = jnp.concatenate([jnp.where(first, low, zero), jnp.where(first, high, zero)], axis=1)
    bottom = jnp.concatenate([jnp.where(first, zero, low), jnp.where(first, zero, high)], axis=1)
    return jnp.concatenate([top, bottom], axis=0)


def solve_windows(pa, pb, za, zb, pivots_row):
    alo, ahi = halves(pa, pb)
    wide = jnp.concatenate([alo, ahi], axis=1)
    of_a = lax.broadcasted_iota(jnp.int32, (64, 256), 1) % 128 < 64

    def spread_rows(x):
        zero = jnp.zeros((64, 256), x.dtype)
        return jnp.concatenate(
            [jnp.where(of_a, x[:64], zero), jnp.where(of_a, zero, x[:64]), jnp.where(of_a, x[64:], zero), jnp.where(of_a, zero, x[64:])],
            axis=0,
        )

    wide_terms = three_terms(wide)
    joint_terms = [spread_rows(t) for t in wide_terms]
    joint_hi, joint_lo = joint_terms[:2]
    first = lax.broadcasted_iota(jnp.int32, (8, 128), 1) < 64
    row = lax.broadcasted_iota(jnp.int32, (8, 128), 0)
    pick = (jnp.where((row == 0) & first, 1.0, 0.0) + jnp.where((row == 1) & (~first), 1.0, 0.0)).astype(jnp.bfloat16)
    j = lax.broadcasted_iota(jnp.int32, (256, 128), 0)
    lane = lax.broadcasted_iota(jnp.int32, (256, 128), 1)
    own = (j // 64) % 2 == lane // 64
    dim = j % 64 + 64 * (j // 128)
    onehot = jnp.where(own & (dim == pivots_row), 1.0, 0.0).astype(jnp.bfloat16)
    r = lax.broadcasted_iota(jnp.int32, (64, 128), 0)
    c = lax.broadcasted_iota(jnp.int32, (64, 128), 1)
    diagonal = c % 64 == r
    z_hi, z_lo = two_terms(jnp.concatenate(halves(za, zb), axis=1))
    square = dot_full([t[:64] for t in wide_terms], joint_terms)
    low, high = whiten(None, square[:, :128], square[:, 128:])
    image = three_terms(jnp.concatenate([low, high], axis=1))
    gram = dot_full(image, [masked_pair(t[:, :128], t[:, 128:]) for t in image], NT)
    low, high = whiten(gram, low, high)
    basis = jnp.concatenate([low, high], axis=1)
    basis_hi, basis_lo = two_terms(basis)
    both = jnp.concatenate([basis_hi, basis_lo], axis=0)
    image = dot_bf16(both, joint_hi)
    image = image[:64] + (image[64:] + dot_bf16(basis_hi, joint_lo))
    prod = low * image[:, :128] + high * image[:, 128:]
    prod_hi, prod_lo = two_terms(prod)
    squares = dot_bf16(pick, prod_hi, NT) + dot_bf16(pick, prod_lo, NT)
    picked = dot_bf16(both, onehot)
    picked = picked[:64] + picked[64:]
    weight = jnp.sum(jnp.where(diagonal, picked, 0.0), axis=0, keepdims=True) * math.sqrt(128)
    pair_hi, pair_lo = masked_pair(basis_hi[:, :128], basis_hi[:, 128:]), masked_pair(basis_lo[:, :128], basis_lo[:, 128:])
    proj = dot_bf16(jnp.concatenate([z_hi, z_lo], axis=0), pair_hi, NT)
    proj = (proj[:32] + (proj[32:] + dot_bf16(z_hi, pair_lo, NT))) * weight
    return jnp.sqrt(squares[:2]), proj


MESH = pl.DeviceIdType.MESH
CHUNKS = 8


def rdma(src, dst, send, recv, where):
    return pltpu.make_async_remote_copy(
        src_ref=src, dst_ref=dst, send_sem=send, recv_sem=recv, device_id=where, device_id_type=MESH
    )


def gram_of(x):
    return lax.dot_general(
        x, x, (((0,), (0,)), ((), ())), precision=lax.Precision.HIGHEST, preferred_element_type=jnp.float32
    )


def gram_split(x):
    high = x.astype(jnp.bfloat16)
    low = (x - high.astype(jnp.float32)).astype(jnp.bfloat16)
    both = jnp.concatenate([high, low], axis=1)
    g = lax.dot_general(both, both, (((0,), (0,)), ((), ())), preferred_element_type=jnp.float32)
    return (g[:128, :128] + g[128:, 128:]) + (g[:128, 128:] + g[128:, :128])


def slot_of(q):
    return lax.rem(q, 2) * 8 + q // 2


def sum_kernel(snap_hbm, sketch_hbm, own_ref, grams_ref,
               snap, sketch, part, rs_buf, ag_buf, gath, gram_send, gram_recv,
               in_sem, rs_send, rs_recv, ag_send, ag_recv, ag_other, xy_send, xy_recv, pair_sem):
    d = lax.axis_index("dof")
    w = lax.axis_index("win")
    nd, nw = 16, 16
    core = lax.rem(d, 2)
    partner = d + 1 - 2 * core
    depth = sketch.shape[0] // CHUNKS
    for i in range(CHUNKS):
        rows = pl.ds(i * depth, depth)
        pltpu.make_async_copy(sketch_hbm.at[rows, :], sketch.at[rows, :], in_sem.at[i]).start()
        pltpu.make_async_copy(snap_hbm.at[:, rows], snap.at[:, rows], in_sem.at[i]).start()
    gath[...] = jnp.zeros_like(gath)
    barrier = pltpu.get_barrier_semaphore()
    for k in range(1, 16):
        pl.semaphore_signal(barrier, inc=1, device_id={"dof": lax.rem(d + k, nd)}, device_id_type=MESH)
        pl.semaphore_signal(barrier, inc=1, device_id={"win": lax.rem(w + k, nw)}, device_id_type=MESH)
    total = jnp.zeros((64, 128), jnp.float32)
    chunk_bytes = pl.ds(0, depth + depth // 2)
    for i in range(CHUNKS):
        rows = pl.ds(i * depth, depth)
        pltpu.make_async_copy(sketch_hbm.at[chunk_bytes, :], sketch.at[chunk_bytes, :], in_sem.at[i]).wait()
        total = total + jnp.dot(snap[:, rows], sketch[rows, :], preferred_element_type=jnp.float32)
    for p in range(16):
        part[p] = total[4 * p : 4 * p + 4, :]
    pl.semaphore_wait(barrier, 30)
    me = slot_of(d)
    order = [8, 9, 7, 6, 10, 5, 11, 4, 12, 3, 13, 2, 14, 15, 1]
    for k in order:
        q = lax.rem(d + k, nd)
        rdma(part.at[slot_of(q)], rs_buf.at[me], rs_send, rs_recv, {"dof": q}).start()
    rs_buf[me] = part[me]
    fifteen = pl.ds(0, 15)
    rdma(part.at[fifteen], rs_buf.at[fifteen], rs_send, rs_recv, {"dof": partner}).wait_recv()
    ag_buf[me] = jnp.sum(rs_buf[...], axis=0)
    z_here = d // 2
    for k in order:
        q = lax.rem(d + k, nd)
        arrival = ag_other if k % 2 else ag_recv.at[z_here]
        rdma(ag_buf.at[me], ag_buf.at[me], ag_send, arrival, {"dof": q}).start()

    def wait_piece(q):
        rdma(ag_buf.at[slot_of(q)], ag_buf.at[slot_of(q)], ag_send, ag_recv.at[q // 2], {"dof": q}).wait_recv()

    def forward(first, count):
        src = ag_buf.at[pl.ds(core * 8 + first, count)]
        dst = gath.at[w, pl.ds(first, count)]

        def send(v, carry):
            rdma(src, dst, xy_send, xy_recv, {"win": v}).start()
            return carry

        lax.fori_loop(w + 1, 16, send, 0)

    forward(z_here, 1)
    for k in reversed(order):
        if k % 2 == 0:
            q = lax.rem(d + k, nd)
            wait_piece(q)
            forward(q // 2, 1)
    eight = pl.ds(0, 8)
    rdma(ag_buf.at[eight], ag_buf.at[eight], ag_send, ag_other, {"dof": partner}).wait_recv()
    own = ag_buf[...].reshape(64, 128)
    own_ref[...] = own
    ma = gram_of(own[:32])
    mab = ma + gram_of(own[32:])
    eye = jnp.where(
        lax.broadcasted_iota(jnp.int32, (128, 128), 0) == lax.broadcasted_iota(jnp.int32, (128, 128), 1), 1.0, 0.0
    )
    count = jnp.full((128, 128), 64 * w, jnp.int32).astype(jnp.float32)
    inv_a, inv_b = 1.0 / (count + 32.0), 1.0 / (count + 64.0)
    own_a, own_b = eye + ma * inv_a, eye + mab * inv_b

    def blocks(count):
        some = gath.at[pl.ds(0, count)]
        return rdma(some, some, xy_send, xy_recv, {"dof": partner})

    for count in range(1, 16):
        @pl.when(w == count)
        def _():
            blocks(count).wait_recv()
    gram_send[...] = gram_split(gath[...].reshape(512, 128))
    swap = rdma(gram_send, gram_recv, pair_sem.at[0], pair_sem.at[1], {"dof": partner})
    swap.start()
    rdma(part.at[fifteen], rs_buf.at[fifteen], rs_send, rs_recv, {"dof": partner}).wait_send()
    rdma(ag_buf.at[fifteen], ag_buf.at[fifteen], ag_send, ag_other, {"dof": partner}).wait_send()
    for count in range(1, 16):
        @pl.when(w == 15 - count)
        def _():
            blocks(count).wait_send()
    swap.wait()
    base = gram_send[...] + gram_recv[...]
    grams_ref[0] = own_a + base * inv_a
    grams_ref[1] = own_b + base * inv_b


def sum_call(snapshots, sketch_matrix):
    depth = sketch_matrix.shape[0] // CHUNKS
    f32 = jnp.float32
    return pl.pallas_call(
        sum_kernel,
        out_shape=(jax.ShapeDtypeStruct((64, 128), f32), jax.ShapeDtypeStruct((2, 128, 128), f32)),
        in_specs=[pl.BlockSpec(memory_space=pl.ANY)] * 2,
        out_specs=(pl.BlockSpec(memory_space=pltpu.VMEM),) * 2,
        scratch_shapes=[
            pltpu.VMEM((64, CHUNKS * depth), jnp.bfloat16),
            pltpu.VMEM((CHUNKS * depth, 128), jnp.bfloat16),
            pltpu.VMEM((16, 4, 128), f32),
            pltpu.VMEM((16, 4, 128), f32),
            pltpu.VMEM((16, 4, 128), f32),
            pltpu.VMEM((16, 8, 4, 128), f32),
            pltpu.VMEM((128, 128), f32),
            pltpu.VMEM((128, 128), f32),
            pltpu.SemaphoreType.DMA((CHUNKS,)),
            pltpu.SemaphoreType.DMA,
            pltpu.SemaphoreType.DMA,
            pltpu.SemaphoreType.DMA,
            pltpu.SemaphoreType.DMA((8,)),
            pltpu.SemaphoreType.DMA,
            pltpu.SemaphoreType.DMA,
            pltpu.SemaphoreType.DMA,
            pltpu.SemaphoreType.DMA((2,)),
        ],
        compiler_params=pltpu.CompilerParams(collective_id=0, has_side_effects=True, vmem_limit_bytes=52 * 1024 * 1024),
    )(snapshots.T, sketch_matrix)

def solve_kernel(own_ref, grams_ref, pivots_ref, sing_ref, proj_ref):
    piv = pivots_ref[...]
    piv_row = jnp.concatenate([piv[0:1, :], piv[1:2, :]], axis=1)
    sing, proj = solve_windows(grams_ref[0], grams_ref[1], own_ref[:32, :], own_ref[32:, :], piv_row)
    sing_ref[...] = sing
    proj_ref[0] = proj[:, :64]
    proj_ref[1] = proj[:, 64:]


def local(snapshots, sketch_matrix, pivots):
    own, grams = sum_call(snapshots, sketch_matrix)
    sing, proj = pl.pallas_call(
        solve_kernel,
        out_shape=(jax.ShapeDtypeStruct((2, 64), jnp.float32), jax.ShapeDtypeStruct((2, 32, 64), jnp.float32)),
        in_specs=[pl.BlockSpec(memory_space=pltpu.VMEM)] * 3,
        out_specs=(pl.BlockSpec(memory_space=pltpu.VMEM),) * 2,
        compiler_params=pltpu.CompilerParams(vmem_limit_bytes=16 * 1024 * 1024),
    )(own, grams, pivots)
    return sing, jnp.swapaxes(proj, 1, 2)


def solution(mesh):
    placed = (P("dof", "win"), P("dof", None), P("win", None))
    return jax.shard_map(
        local,
        mesh=mesh,
        in_specs=placed,
        out_specs=(P("win", None), P("win", None, None)),
        check_vma=False,
    )
```
